32 devices in a mesh: tok: 16 (over z, x, core), head: 2 (over y).
Axes of the slice: x: 2, y: 2, z: 4, core: 2. Of those that a mesh axis runs over, the one named last changes fastest.
Arguments:
- inputs: bfloat16 [2, 8192, 2048], P(None, 'tok'), may hold values from -6 to 6
- projections: bfloat16 [3, 2048, 2048], P(None, None, 'head'), may hold values from -0.125 to 0.125
- lrate: float32 [2, 8192, 4], P(None, 'tok', 'head'), may hold values from 0.1 to 1
- fast_init: bfloat16 [4, 3, 384, 512], P('head'), may hold values from -0.25 to 0.25
- gain: float32 [2048], replicated, may hold values from 0.5 to 1.5
Outputs:
- normed: bfloat16 [2, 8192, 2048], P(None, ('tok', 'head'))
The draws below stay inside these ranges and needn't reach their ends.
All inputs are finite; a program needn't handle non-finite values.
Results may differ from the reference program's by a relative error of at most 0.018.
Values may be sent and summed in bfloat16 or wider, within the bound.
A program may use at most 128 MiB of HBM per device.

```python
import math
import jax
import jax.numpy as jnp
from jax import lax

D = 2048
HEADS = 4
HD = 512
F = 384
INNER = 2
GROUPS = 2
TOKENS = 8192


def block_scale(key, shape, cuts, low, largest):
    factor_of, own = 1.0, jax.random.fold_in(key, 6)
    for position, shards_of in cuts:
        heights = jnp.exp(jax.random.uniform(jax.random.fold_in(own, position), (shards_of,), jnp.float32, low / len(cuts), largest / len(cuts)))
        factor_of = factor_of * jnp.repeat(heights, shape[position] // shards_of).reshape([-1 if axis == position else 1 for axis in range(len(shape))])
    return factor_of


def bell_draw(stream_key, shape, spread, most, pieces=(), kind=jnp.bfloat16):
    loudness = block_scale(stream_key, shape, pieces, -0.22, 0.18) if pieces else 1.0
    drawn = jax.random.normal(stream_key, shape, jnp.float32) * spread * loudness
    return jnp.minimum(jnp.maximum(drawn, -most), most).astype(kind)


def setup_inputs(seed: int = 0) -> dict:
    arg_keys = jax.random.split(jax.random.key(seed), 6)
    inputs = bell_draw(arg_keys[0], (GROUPS, TOKENS, D), 1.0, 6.0, ((1, 16),))
    projections = bell_draw(arg_keys[1], (3, D, D), D ** -0.5, 0.125, ((2, 2),))
    lrate = jnp.clip(jnp.exp(math.log(1.0) - 2.3025851 * jax.random.uniform(arg_keys[2], (GROUPS, TOKENS, HEADS), jnp.float32) ** block_scale(arg_keys[2], (GROUPS, TOKENS, HEADS), ((1, 16), (2, 2)), -0.2, 0.2)), 0.1, 1.0)
    fast_init = bell_draw(arg_keys[3], (HEADS, 3, F, HD), HD ** -0.5, 0.25, ((0, 2),))
    gain = jnp.clip(1.0 + 0.1 * jax.random.normal(arg_keys[4], (D,), jnp.float32), 0.5, 1.5)
    return dict(inputs=inputs, projections=projections, lrate=lrate, fast_init=fast_init, gain=gain)


step_size = 4.0

def mult(form, left, right):
    return jnp.einsum(form, left.astype(jnp.float32), right.astype(jnp.float32))

def silu_parts(hidden):
    sigma = jax.nn.sigmoid(hidden)
    return (hidden * sigma, sigma * (1.0 + hidden * (1.0 - sigma)))

def token_gradients(weights, keys, values, rates):
    hidden = mult('htd,hfd->htf', keys, weights[:, 0])
    gated = mult('htd,hfd->htf', keys, weights[:, 1])
    act, slope = silu_parts(hidden)
    mixed = (act * gated).astype(jnp.bfloat16)
    signal = (-rates[:, :, None] * values.astype(jnp.float32)).astype(jnp.bfloat16)
    grad_second = mult('htf,htd->hfd', mixed, signal)
    back = mult('htd,hfd->htf', signal, weights[:, 2])
    grad_gate = (back * act).astype(jnp.bfloat16)
    grad_first = (back * gated * slope).astype(jnp.bfloat16)
    grad_one = mult('htf,htd->hfd', grad_first, keys)
    grad_three = mult('htf,htd->hfd', grad_gate, keys)
    return jnp.stack([grad_one, grad_three, grad_second], axis=1)

def refresh(weights, summed, target):
    frob = lax.optimization_barrier(jnp.sum(summed * summed, axis=(2, 3)))
    scale = step_size / jnp.sqrt(frob + 1e-06)
    update = weights.astype(jnp.float32) - scale[:, :, None, None] * summed
    length = jnp.sqrt(lax.optimization_barrier(jnp.sum(update * update, axis=-1, keepdims=True)) + 1e-06)
    return (update * (target / length)).astype(jnp.bfloat16)

def read_memory(weights, queries):
    hidden = mult('htd,hfd->htf', queries, weights[:, 0])
    gated = mult('htd,hfd->htf', queries, weights[:, 1])
    act, _ = silu_parts(hidden)
    mixed = (act * gated).astype(jnp.bfloat16)
    return mult('htf,hfd->htd', mixed, weights[:, 2]).astype(jnp.bfloat16)

def reference(inputs, projections, lrate, fast_init, gain):
    target = jnp.sqrt(lax.optimization_barrier(jnp.sum(jnp.square(fast_init.astype(jnp.float32)), axis=-1, keepdims=True)))
    weights = fast_init
    outputs = []
    for group in range(GROUPS):
        mapped = mult('td,sde->ste', inputs[group], projections).astype(jnp.bfloat16)
        split = mapped.reshape(3, TOKENS, HEADS, HD).transpose(0, 2, 1, 3)
        queries, keys, values = (split[0], split[1], split[2])
        rates = lrate[group].T
        for inner in range(INNER):
            summed = token_gradients(weights, keys, values, rates)
            weights = refresh(weights, summed, target)
        readout = read_memory(weights, queries)
        joined = readout.transpose(1, 0, 2).reshape(TOKENS, HEADS * HD).astype(jnp.float32)
        square_mean = lax.optimization_barrier(jnp.mean(joined * joined, axis=-1, keepdims=True))
        outputs.append((joined * lax.rsqrt(square_mean + 1e-06) * gain).astype(jnp.bfloat16))
    return jnp.stack(outputs)
```

```python
import functools

import jax
import jax.numpy as jnp
from jax import lax
from jax.experimental import pallas as pl
from jax.experimental.pallas import tpu as pltpu
from jax.sharding import PartitionSpec as P

INNER = 2
CORES = 2
PAIR = 2
PARTS = 4
HALVES = 2
STEP_SIZE = 4.0
EPS = 1e-06
MESH = pl.DeviceIdType.MESH
BLOCK = 16
LANES = 128
NT = (((1,), (1,)), ((), ()))
F32, BF16 = jnp.float32, jnp.bfloat16


def dot(left, right):
    return jnp.dot(left, right, preferred_element_type=F32)


def dot_nt(left, right):
    return lax.dot_general(left, right, NT, preferred_element_type=F32)


def train_kernel(
    tok_size, head_size,
    x_hbm, w_hbm, lr_ref, init_hbm, out_ref,
    x, w, rate, feat, weights, target, hid, gat, bak, mixed, dgate, dfirst,
    grads, in_recv, partial, mid_recv, whole, sumsq, ro_send,
    load_sem, x_sem, own_sem, fwd_sem, red_sem, w_sem, ro_sem,
):
    groups, tokens, depth = x.shape
    units, width = weights.shape[1], weights.shape[2]
    half = units // CORES
    piece = half // PARTS
    everyone = PAIR * CORES * tokens
    stripe = tokens // HALVES
    quarter = tokens // head_size
    lines = tok_size // (CORES * PAIR)
    reach = lines // 2

    tok, head = lax.axis_index("tok"), lax.axis_index("head")
    core, chip = tok % CORES, tok // CORES
    col, line = chip % PAIR, chip // PAIR
    low = line < reach
    pos = jnp.where(low, line, lines - 1 - line)
    inward = jnp.where(low, 1, -1)
    center, end = pos == reach - 1, pos == 0

    def device(line_, col_, core_, head_):
        return {"tok": (line_ * PAIR + col_) * CORES + core_, "head": head_}

    partner = device(line, col, 1 - core, head)
    across = device(line, 1 - col, core, head)
    inner = device(line + inward, col, core, head)
    outer = device((line - inward + lines) % lines, col, core, head)

    def readers(b):
        dx, dy = 1 - b // head_size, head_size - 1 - b % head_size
        return (col + dx) % PAIR, (head + dy) % head_size

    last_block = PAIR * head_size - 1

    def remote(source, destination, send, recv, to):
        return pltpu.make_async_remote_copy(
            src_ref=source, dst_ref=destination, send_sem=send, recv_sem=recv, device_id=to, device_id_type=MESH
        )

    loads = [pltpu.make_async_copy(x_hbm.at[0], x.at[0], load_sem.at[0])]
    order = [(1, 0), (2, 0), (1, 1), (2, 1), (0, 0), (0, 1)]
    for i, (s, own) in enumerate(order):
        start = pl.multiple_of((col if own else 1 - col) * width, LANES)
        loads.append(pltpu.make_async_copy(
            w_hbm.at[s, :, pl.ds(start, width)], w.at[s, own], load_sem.at[1 + i]))
    for g in range(1, groups):
        loads.append(pltpu.make_async_copy(x_hbm.at[g], x.at[g], load_sem.at[7 + g]))
    own_units = pl.ds(pl.multiple_of(core * half, BLOCK), half)
    load_init = pltpu.make_async_copy(
        init_hbm.at[col, :, own_units], weights.at[:, own_units], load_sem.at[7])
    for copy in loads[:5] + [load_init] + loads[5:]:
        copy.start()

    barrier = pltpu.get_barrier_semaphore()
    pl.semaphore_signal(barrier, inc=1, device_id=partner, device_id_type=MESH)
    pl.semaphore_signal(barrier, inc=1, device_id=inner, device_id_type=MESH)
    for b in range(last_block):
        there, row = readers(b)
        pl.semaphore_signal(barrier, inc=1, device_id=device(line, there, core, row), device_id_type=MESH)
    pl.semaphore_signal(barrier, inc=1, device_id=outer, device_id_type=MESH)

    for g in range(groups):
        for own in range(2):
            which = col if own else 1 - col
            row = lr_ref[g, pl.ds(which, 1), :]
            rate[g, own] = -jnp.transpose(jnp.broadcast_to(row, (LANES, tokens)))

    def stripe_rows(h):
        return pl.ds(pl.multiple_of(h * stripe, stripe), stripe)

    mine, theirs = col * CORES + core, (1 - col) * CORES + core
    parcel = PAIR * CORES

    def project(g, s, own, h):
        rows = stripe_rows(h)
        got = dot(x[g, rows, :], w[s, own]).astype(BF16).astype(F32)
        factor = jnp.where(s == 2, rate[g, own, rows, :], 1.0)
        slot = mine if own else parcel
        for j in range(width // LANES):
            columns = slice(j * LANES, (j + 1) * LANES)
            feat[s, g, slot, rows, columns] = (got[:, columns] * factor).astype(BF16)

    def across_copy(g, s, h):
        rows = stripe_rows(h)
        return remote(feat.at[s, g, parcel, rows], feat.at[s, g, mine, rows],
                      x_sem.at[0, s, g, h], x_sem.at[1, s, g, h], across)

    def own_copy(g, s, h):
        at = feat.at[s, g, mine, stripe_rows(h)]
        return remote(at, at, own_sem.at[0, s, g, h], own_sem.at[1, s, g, h], partner)

    def forward_copy(g, s, h):
        at = feat.at[s, g, theirs, stripe_rows(h)]
        return remote(at, at, fwd_sem.at[0, s, g, h], fwd_sem.at[1, s, g, h], partner)

    def each(count, work):
        def one(i, carry):
            work(i)
            return carry

        lax.fori_loop(0, count, one, 0)

    pl.semaphore_wait(barrier, 3 + last_block)
    for copy in loads[:3]:
        copy.wait()

    def ship_first(i):
        s, h = 1 + i % 2, i // 2
        project(0, s, 0, h)
        across_copy(0, s, h).start()

    each(2 * HALVES, ship_first)
    for copy in loads[3:5]:
        copy.wait()

    def keep_first(i):
        s, h = 1 + i % 2, i // 2
        project(0, s, 1, h)
        own_copy(0, s, h).start()

    each(2 * HALVES, keep_first)
    load_init.wait()

    def unit_rows(block):
        return pl.ds(pl.multiple_of(core * half + block * BLOCK, BLOCK), BLOCK)

    def block_rows(block):
        return pl.ds(pl.multiple_of(block * BLOCK, BLOCK), BLOCK)

    def prepare(i):
        m, block = i // (half // BLOCK), i % (half // BLOCK)
        start = weights[m, unit_rows(block), :].astype(F32)
        target[m, block_rows(block), :] = jnp.sqrt(jnp.sum(start * start, axis=-1, keepdims=True))

    each(3 * half // BLOCK, prepare)
    for copy in loads[5:]:
        copy.wait()

    def ship_rest(i):
        g, j = 1 + i // (2 * HALVES), i % (2 * HALVES)
        project(g, 1 + j % 2, 0, j // 2)

    each((groups - 1) * 2 * HALVES, ship_rest)

    def keep_rest(i):
        g, j = 1 + i // (2 * HALVES), i % (2 * HALVES)
        s, h = 1 + j % 2, j // 2
        project(g, s, 1, h)
        own_copy(g, s, h).start()

    each((groups - 1) * 2 * HALVES, keep_rest)

    def read_other(i):
        project(i // HALVES, 0, 0, i % HALVES)

    def read_own(i):
        project(i // HALVES, 0, 1, i % HALVES)

    each(groups * HALVES, read_other)
    each(groups * HALVES, read_own)

    def pass_on(g):
        for h in range(HALVES):
            for s in (1, 2):
                across_copy(g, s, h).wait_recv()
                forward_copy(g, s, h).start()

    def settle(g):
        for h in range(HALVES):
            for s in (1, 2):
                own_copy(g, s, h).wait()
                forward_copy(g, s, h).wait()

    pass_on(0)
    for h in range(HALVES):
        for s in (1, 2):
            across_copy(0, s, h).wait_send()
    for g in range(1, groups):
        for h in range(HALVES):
            for s in (1, 2):
                across_copy(g, s, h).start()

    def chunk_rows(k):
        return slice(k * piece, (k + 1) * piece)

    def send_in(m, k, source):
        at = chunk_rows(k)
        return remote(source.at[m, at], in_recv.at[m, at], red_sem.at[0, m, k], red_sem.at[1, m, k], inner)

    def send_mid(step, m, k):
        at = chunk_rows(k)
        source = grads if reach == 1 else partial
        return remote(source.at[m, at], mid_recv.at[step, m, at], red_sem.at[2, m, k], red_sem.at[3 + step, m, k], inner)

    def send_out(m, k):
        at = chunk_rows(k)
        return remote(whole.at[m, at], whole.at[m, at], red_sem.at[5, m, k], red_sem.at[6, m, k], outer)

    def launch(step, m, k):
        @pl.when(end)
        def _():
            if reach == 1:
                send_mid(step, m, k).start()
            else:
                send_in(m, k, grads).start()

    def relay(step, m, k):
        @pl.when(pos > 0)
        def _():
            at = chunk_rows(k)
            send_in(m, k, grads).wait_recv()
            partial[m, at, :] = (grads[m, at, :].astype(F32) + in_recv[m, at, :].astype(F32)).astype(BF16)

            @pl.when(center)
            def _():
                send_mid(step, m, k).start()

            if reach > 2:
                @pl.when(jnp.logical_not(center))
                def _():
                    send_in(m, k, partial).start()

    def finish(step, m, k):
        @pl.when(center)
        def _():
            at = chunk_rows(k)
            send_mid(step, m, k).wait_recv()
            source = grads if reach == 1 else partial
            whole[m, at, :] = (source[m, at, :].astype(F32) + mid_recv[step, m, at, :].astype(F32)).astype(BF16)
            if reach > 1:
                send_out(m, k).start()

    def collect(m):
        if reach > 1:
            @pl.when(jnp.logical_not(center))
            def _():
                for k in range(PARTS):
                    send_out(m, k).wait_recv()
                    if reach > 2:
                        @pl.when(pos > 0)
                        def _(k=k):
                            send_out(m, k).start()

    def drain(step, m):
        for k in range(PARTS):
            @pl.when(center)
            def _(k=k):
                send_mid(step, m, k).wait_send()

            if reach > 1:
                @pl.when(jnp.logical_not(center))
                def _(k=k):
                    send_in(m, k, grads).wait_send()

                @pl.when(pos > 0)
                def _(k=k):
                    send_out(m, k).wait_send()

    def share_square(step, m):
        return remote(sumsq.at[step, 0, m], sumsq.at[step, 1, m], red_sem.at[7, m, 0], red_sem.at[8 + step, m, 0], partner)

    def measure(step, m):
        collect(m)
        total = jnp.zeros((BLOCK, width), F32)
        for block in range(half // BLOCK):
            part = whole[m, block * BLOCK:(block + 1) * BLOCK, :].astype(F32)
            total = total + part * part
        total = total[:8] + total[8:]
        sumsq[step, 0, m] = sum(total[:, j * LANES:(j + 1) * LANES] for j in range(width // LANES))
        share_square(step, m).start()

    def update_memory(step, m):
        share_square(step, m).wait()
        both = sumsq[step, 0, m] + sumsq[step, 1, m]
        frob = jnp.sum(jnp.sum(both, axis=0, keepdims=True), axis=1, keepdims=True)
        scale = STEP_SIZE / jnp.sqrt(frob + EPS)

        def refresh(block):
            at, here = unit_rows(block), block_rows(block)
            update = weights[m, at, :].astype(F32) - scale * whole[m, here, :].astype(F32)
            length = jnp.sqrt(jnp.sum(update * update, axis=-1, keepdims=True) + EPS)
            weights[m, at, :] = (update * (target[m, here, :] / length)).astype(BF16)

        each(half // BLOCK, refresh)

    def share_memory(m):
        at = weights.at[m, own_units]
        return remote(at, at, w_sem.at[0, m], w_sem.at[1, m], partner)

    def all_tokens(s, g):
        return feat[s, g, :parcel].reshape(everyone, width)

    def read_copy(g, b):
        there, row = readers(b)
        return remote(ro_send.at[g, b], out_ref.at[g, head * PAIR + col],
                      ro_sem.at[0, g, b], ro_sem.at[1, g, b], device(line, there, core, row))

    def read_block(g, b):
        there, row = readers(b)
        queries = feat[0, g, there * CORES + core, pl.ds(pl.multiple_of(row * quarter, BLOCK), quarter), :]
        hidden, gated = dot_nt(queries, weights[0]), dot_nt(queries, weights[1])
        readmix = (hidden * jax.nn.sigmoid(hidden) * gated).astype(BF16)
        return dot(readmix, weights[2]).astype(BF16)

    def read_ship(g, b):
        ro_send[g, b] = read_block(g, b)
        read_copy(g, b).start()

    def read_keep(g):
        out_ref[g, head * PAIR + col] = read_block(g, last_block)

    def read_ready(g):
        for m in range(3):
            share_memory(m).wait()
        for h in range(HALVES):
            across_copy(g, 0, h).wait()

    stages = (2, 1, 0)

    def inner_step(g, step):
        keys, signal = all_tokens(1, g), all_tokens(2, g)
        own_first, own_third, own_second = (weights[m, own_units, :] for m in range(3))
        hid[...] = dot_nt(own_first, keys)
        gat[...] = dot_nt(own_third, keys)
        bak[...] = dot_nt(own_second, signal)
        strips = 4
        strip = everyone // strips

        def pointwise(i):
            at = block_rows(i // strips), pl.ds(pl.multiple_of((i % strips) * strip, LANES), strip)
            hidden, gated, back = hid[at], gat[at], bak[at]
            sigma = jax.nn.sigmoid(hidden)
            act = hidden * sigma
            mixed[at] = (act * gated).astype(BF16)
            dgate[at] = (back * act).astype(BF16)
            dfirst[at] = (back * gated * (sigma * (1.0 + hidden * (1.0 - sigma)))).astype(BF16)

        each(half // BLOCK * strips, pointwise)
        factors = {2: (mixed, signal), 1: (dgate, keys), 0: (dfirst, keys)}
        for m in stages:
            left, right = factors[m]
            grads[m] = dot(left[...], right).astype(BF16)
            for k in range(PARTS):
                launch(step, m, k)

        chunks = [(m, k) for m in stages for k in range(PARTS)]
        skew, lag = 2, 2
        for turn in range(len(chunks) + skew + lag):
            if turn < len(chunks):
                relay(step, *chunks[turn])
            if 0 <= turn - skew < len(chunks):
                m, k = chunks[turn - skew]
                finish(step, m, k)
                if k == PARTS - 1:
                    measure(step, m)
            if 0 <= turn - skew - lag < len(chunks):
                m, k = chunks[turn - skew - lag]
                if k == PARTS - 1:
                    update_memory(step, m)
                    if step == INNER - 1:
                        share_memory(m).start()
            if step == 0 and turn == 0:
                @pl.when(g > 0)
                def _():
                    read_ready(g - 1)
            if step == 0 and turn < last_block:
                @pl.when(g > 0)
                def _(turn=turn):
                    read_ship(g - 1, turn)
            if step == 0 and turn == last_block:
                @pl.when(g > 0)
                def _():
                    read_keep(g - 1)
            if step == INNER - 1 and turn == 0:
                for h in range(HALVES):
                    across_copy(g, 0, h).start()
            if step == INNER - 1 and turn == 5:
                @pl.when(g < groups - 1)
                def _():
                    pass_on(g + 1)
        for m in stages:
            drain(step, m)

    def group(g):
        settle(g)

        @pl.when(g > 0)
        def _():
            for h in range(HALVES):
                for s in (1, 2):
                    across_copy(g, s, h).wait_send()

        for step in range(INNER):
            inner_step(g, step)

    each(groups, group)
    read_ready(groups - 1)
    each(last_block, lambda b: read_ship(groups - 1, b))
    read_keep(groups - 1)

    def land(i):
        read_copy(i // last_block, i % last_block).wait()

    each(groups * last_block, land)


def solution(mesh):
    tok_size, head_size = mesh.shape["tok"], mesh.shape["head"]

    def body(inputs, projections, lrate, fast_init, gain):
        groups, tokens, depth = inputs.shape
        heads, _, units, width = fast_init.shape
        assert heads == PAIR and INNER == 2
        half = units // CORES
        everyone = PAIR * CORES * tokens
        quarter = tokens // head_size
        all_heads = PAIR * head_size
        parts = pl.pallas_call(
            functools.partial(train_kernel, tok_size, head_size),
            out_shape=jax.ShapeDtypeStruct((groups, all_heads, quarter, width), BF16),
            in_specs=[
                pl.BlockSpec(memory_space=pl.ANY),
                pl.BlockSpec(memory_space=pl.ANY),
                pl.BlockSpec(memory_space=pltpu.VMEM),
                pl.BlockSpec(memory_space=pl.ANY),
            ],
            out_specs=pl.BlockSpec(memory_space=pltpu.VMEM),
            scratch_shapes=[
                pltpu.VMEM((groups, tokens, depth), BF16),
                pltpu.VMEM((3, 2, depth, width), BF16),
                pltpu.VMEM((groups, 2, tokens, LANES), F32),
                pltpu.VMEM((3, groups, PAIR * CORES + 1, tokens, width), BF16),
                pltpu.VMEM((3, units, width), BF16),
                pltpu.VMEM((3, half, 1), F32),
                pltpu.VMEM((half, everyone), F32),
                pltpu.VMEM((half, everyone), F32),
                pltpu.VMEM((half, everyone), F32),
                pltpu.VMEM((half, everyone), BF16),
                pltpu.VMEM((half, everyone), BF16),
                pltpu.VMEM((half, everyone), BF16),
                pltpu.VMEM((3, half, width), BF16),
                pltpu.VMEM((3, half, width), BF16),
                pltpu.VMEM((3, half, width), BF16),
                pltpu.VMEM((INNER, 3, half, width), BF16),
                pltpu.VMEM((3, half, width), BF16),
                pltpu.VMEM((INNER, 2, 3, 8, LANES), F32),
                pltpu.VMEM((groups, all_heads - 1, quarter, width), BF16),
                pltpu.SemaphoreType.DMA((7 + groups,)),
                pltpu.SemaphoreType.DMA((2, 3, groups, HALVES)),
                pltpu.SemaphoreType.DMA((2, 3, groups, HALVES)),
                pltpu.SemaphoreType.DMA((2, 3, groups, HALVES)),
                pltpu.SemaphoreType.DMA((8 + INNER, 3, PARTS)),
                pltpu.SemaphoreType.DMA((2, 3)),
                pltpu.SemaphoreType.DMA((2, groups, all_heads - 1)),
            ],
            compiler_params=pltpu.CompilerParams(
                collective_id=0, has_side_effects=True, vmem_limit_bytes=60000 * 1024
            ),
        )(inputs, projections, lrate.transpose(0, 2, 1), fast_init)
        parts = parts.astype(F32)
        square = jnp.sum(parts * parts, axis=(1, 3), keepdims=True)
        factor = lax.rsqrt(square / (all_heads * width) + EPS)
        normed = (parts * factor * gain.reshape(1, all_heads, 1, width)).astype(BF16)
        return normed.transpose(0, 2, 1, 3).reshape(groups, quarter, all_heads * width)

    return jax.shard_map(
        body,
        mesh=mesh,
        in_specs=(
            P(None, "tok", None),
            P(None, None, "head"),
            P(None, "tok", "head"),
            P("head", None, None, None),
            P(),
        ),
        out_specs=P(None, ("tok", "head"), None),
        check_vma=False,
    )
```

```python
import functools

import jax
import jax.numpy as jnp
from jax import lax
from jax.experimental import pallas as pl
from jax.experimental.pallas import tpu as pltpu
from jax.sharding import PartitionSpec as P

INNER = 2
CORES = 2
PAIR = 2
PARTS = 4
HALVES = 2
STEP_SIZE = 4.0
EPS = 1e-06
MESH = pl.DeviceIdType.MESH
BLOCK = 16
LANES = 128
NORM_ROWS = 256
NT = (((1,), (1,)), ((), ()))
F32, BF16 = jnp.float32, jnp.bfloat16


def dot(left, right):
    return jnp.dot(left, right, preferred_element_type=F32)


def dot_nt(left, right):
    return lax.dot_general(left, right, NT, preferred_element_type=F32)


def train_kernel(
    tok_size, head_size,
    x_hbm, w_hbm, lr_ref, init_hbm, out_ref,
    x, w, rate, feat, weights, target, hid, gat, bak, mixed, dgate, dfirst,
    grads, in_recv, partial, mid_recv, whole, sumsq, ro_send,
    load_sem, x_sem, own_sem, fwd_sem, red_sem, w_sem, ro_sem,
):
    groups, tokens, depth = x.shape
    units, width = weights.shape[1], weights.shape[2]
    half = units // CORES
    piece = half // PARTS
    everyone = PAIR * CORES * tokens
    stripe = tokens // HALVES
    quarter = tokens // head_size
    lines = tok_size // (CORES * PAIR)
    reach = lines // 2

    tok, head = lax.axis_index("tok"), lax.axis_index("head")
    core, chip = tok % CORES, tok // CORES
    col, line = chip % PAIR, chip // PAIR
    low = line < reach
    pos = jnp.where(low, line, lines - 1 - line)
    inward = jnp.where(low, 1, -1)
    center, end = pos == reach - 1, pos == 0

    def device(line_, col_, core_, head_):
        return {"tok": (line_ * PAIR + col_) * CORES + core_, "head": head_}

    partner = device(line, col, 1 - core, head)
    across = device(line, 1 - col, core, head)
    inner = device(line + inward, col, core, head)
    outer = device((line - inward + lines) % lines, col, core, head)

    def readers(b):
        dx, dy = 1 - b // head_size, head_size - 1 - b % head_size
        return (col + dx) % PAIR, (head + dy) % head_size

    last_block = PAIR * head_size - 1

    def remote(source, destination, send, recv, to):
        return pltpu.make_async_remote_copy(
            src_ref=source, dst_ref=destination, send_sem=send, recv_sem=recv, device_id=to, device_id_type=MESH
        )

    loads = [pltpu.make_async_copy(x_hbm.at[0], x.at[0], load_sem.at[0])]
    order = [(1, 0), (2, 0), (1, 1), (2, 1), (0, 0), (0, 1)]
    for i, (s, own) in enumerate(order):
        start = pl.multiple_of((col if own else 1 - col) * width, LANES)
        loads.append(pltpu.make_async_copy(
            w_hbm.at[s, :, pl.ds(start, width)], w.at[s, own], load_sem.at[1 + i]))
    for g in range(1, groups):
        loads.append(pltpu.make_async_copy(x_hbm.at[g], x.at[g], load_sem.at[7 + g]))
    own_units = pl.ds(pl.multiple_of(core * half, BLOCK), half)
    load_init = pltpu.make_async_copy(
        init_hbm.at[col, :, own_units], weights.at[:, own_units], load_sem.at[7])
    for copy in loads[:5] + [load_init] + loads[5:]:
        copy.start()

    barrier = pltpu.get_barrier_semaphore()
    pl.semaphore_signal(barrier, inc=1, device_id=partner, device_id_type=MESH)
    pl.semaphore_signal(barrier, inc=1, device_id=inner, device_id_type=MESH)
    for b in range(last_block):
        there, row = readers(b)
        pl.semaphore_signal(barrier, inc=1, device_id=device(line, there, core, row), device_id_type=MESH)
    pl.semaphore_signal(barrier, inc=1, device_id=outer, device_id_type=MESH)

    for g in range(groups):
        for own in range(2):
            which = col if own else 1 - col
            row = lr_ref[g, pl.ds(which, 1), :]
            rate[g, own] = -jnp.transpose(jnp.broadcast_to(row, (LANES, tokens)))

    def stripe_rows(h):
        return pl.ds(pl.multiple_of(h * stripe, stripe), stripe)

    mine, theirs = col * CORES + core, (1 - col) * CORES + core
    parcel = PAIR * CORES

    def project(g, s, own, h):
        rows = stripe_rows(h)
        got = dot(x[g, rows, :], w[s, own]).astype(BF16).astype(F32)
        factor = jnp.where(s == 2, rate[g, own, rows, :], 1.0)
        slot = mine if own else parcel
        for j in range(width // LANES):
            columns = slice(j * LANES, (j + 1) * LANES)
            feat[s, g, slot, rows, columns] = (got[:, columns] * factor).astype(BF16)

    def across_copy(g, s, h):
        rows = stripe_rows(h)
        return remote(feat.at[s, g, parcel, rows], feat.at[s, g, mine, rows],
                      x_sem.at[0, s, g, h], x_sem.at[1, s, g, h], across)

    def own_copy(g, s, h):
        at = feat.at[s, g, mine, stripe_rows(h)]
        return remote(at, at, own_sem.at[0, s, g, h], own_sem.at[1, s, g, h], partner)

    def forward_copy(g, s, h):
        at = feat.at[s, g, theirs, stripe_rows(h)]
        return remote(at, at, fwd_sem.at[0, s, g, h], fwd_sem.at[1, s, g, h], partner)

    def each(count, work, unroll=1):
        def one(i, carry):
            work(i)
            return carry

        lax.fori_loop(0, count, one, 0, unroll=unroll)

    pl.semaphore_wait(barrier, 3 + last_block)
    for copy in loads[:3]:
        copy.wait()

    def ship_first(i):
        s, h = 1 + i % 2, i // 2
        project(0, s, 0, h)
        across_copy(0, s, h).start()

    each(2 * HALVES, ship_first)
    for copy in loads[3:5]:
        copy.wait()

    def keep_first(i):
        s, h = 1 + i % 2, i // 2
        project(0, s, 1, h)
        own_copy(0, s, h).start()

    each(2 * HALVES, keep_first)
    load_init.wait()

    def unit_rows(block):
        return pl.ds(pl.multiple_of(core * half + block * BLOCK, BLOCK), BLOCK)

    def block_rows(block):
        return pl.ds(pl.multiple_of(block * BLOCK, BLOCK), BLOCK)

    def prepare(i):
        m, block = i // (half // BLOCK), i % (half // BLOCK)
        start = weights[m, unit_rows(block), :].astype(F32)
        target[m, block_rows(block), :] = jnp.sqrt(jnp.sum(start * start, axis=-1, keepdims=True))

    each(3 * half // BLOCK, prepare, half // BLOCK)
    for copy in loads[5:]:
        copy.wait()

    def ship_rest(i):
        g, j = 1 + i // (2 * HALVES), i % (2 * HALVES)
        project(g, 1 + j % 2, 0, j // 2)

    each((groups - 1) * 2 * HALVES, ship_rest)

    def keep_rest(i):
        g, j = 1 + i // (2 * HALVES), i % (2 * HALVES)
        s, h = 1 + j % 2, j // 2
        project(g, s, 1, h)
        own_copy(g, s, h).start()

    each((groups - 1) * 2 * HALVES, keep_rest)

    def read_other(i):
        project(i // HALVES, 0, 0, i % HALVES)

    def read_own(i):
        project(i // HALVES, 0, 1, i % HALVES)

    each(groups * HALVES, read_other)
    each(groups * HALVES, read_own)

    def pass_on(g):
        for h in range(HALVES):
            for s in (1, 2):
                across_copy(g, s, h).wait_recv()
                forward_copy(g, s, h).start()

    def settle(g):
        for h in range(HALVES):
            for s in (1, 2):
                own_copy(g, s, h).wait()
                forward_copy(g, s, h).wait()

    pass_on(0)
    for h in range(HALVES):
        for s in (1, 2):
            across_copy(0, s, h).wait_send()
    for g in range(1, groups):
        for h in range(HALVES):
            for s in (1, 2):
                across_copy(g, s, h).start()

    def chunk_rows(k):
        return slice(k * piece, (k + 1) * piece)

    def send_in(m, k, source):
        at = chunk_rows(k)
        return remote(source.at[m, at], in_recv.at[m, at], red_sem.at[0, m, k], red_sem.at[1, m, k], inner)

    def send_mid(step, m, k):
        at = chunk_rows(k)
        source = grads if reach == 1 else partial
        return remote(source.at[m, at], mid_recv.at[step, m, at], red_sem.at[2, m, k], red_sem.at[3 + step, m, k], inner)

    def send_out(m, k):
        at = chunk_rows(k)
        return remote(whole.at[m, at], whole.at[m, at], red_sem.at[5, m, k], red_sem.at[6, m, k], outer)

    def launch(step, m, k):
        @pl.when(end)
        def _():
            if reach == 1:
                send_mid(step, m, k).start()
            else:
                send_in(m, k, grads).start()

    def relay(step, m, k):
        @pl.when(pos > 0)
        def _():
            at = chunk_rows(k)
            send_in(m, k, grads).wait_recv()
            partial[m, at, :] = (grads[m, at, :].astype(F32) + in_recv[m, at, :].astype(F32)).astype(BF16)

            @pl.when(center)
            def _():
                send_mid(step, m, k).start()

            if reach > 2:
                @pl.when(jnp.logical_not(center))
                def _():
                    send_in(m, k, partial).start()

    def finish(step, m, k):
        @pl.when(center)
        def _():
            at = chunk_rows(k)
            send_mid(step, m, k).wait_recv()
            source = grads if reach == 1 else partial
            whole[m, at, :] = (source[m, at, :].astype(F32) + mid_recv[step, m, at, :].astype(F32)).astype(BF16)
            if reach > 1:
                send_out(m, k).start()

    def collect(m):
        if reach > 1:
            @pl.when(jnp.logical_not(center))
            def _():
                for k in range(PARTS):
                    send_out(m, k).wait_recv()
                    if reach > 2:
                        @pl.when(pos > 0)
                        def _(k=k):
                            send_out(m, k).start()

    def drain(step, m):
        for k in range(PARTS):
            @pl.when(center)
            def _(k=k):
                send_mid(step, m, k).wait_send()

            if reach > 1:
                @pl.when(jnp.logical_not(center))
                def _(k=k):
                    send_in(m, k, grads).wait_send()

                @pl.when(pos > 0)
                def _(k=k):
                    send_out(m, k).wait_send()

    def share_square(step, m):
        return remote(sumsq.at[step, 0, m], sumsq.at[step, 1, m], red_sem.at[7, m, 0], red_sem.at[8 + step, m, 0], partner)

    def measure(step, m):
        collect(m)
        total = jnp.zeros((BLOCK, width), F32)
        for block in range(half // BLOCK):
            part = whole[m, block * BLOCK:(block + 1) * BLOCK, :].astype(F32)
            total = total + part * part
        total = total[:8] + total[8:]
        sumsq[step, 0, m] = sum(total[:, j * LANES:(j + 1) * LANES] for j in range(width // LANES))
        share_square(step, m).start()

    def update_memory(step, m):
        share_square(step, m).wait()
        both = sumsq[step, 0, m] + sumsq[step, 1, m]
        frob = jnp.sum(jnp.sum(both, axis=0, keepdims=True), axis=1, keepdims=True)
        scale = STEP_SIZE / jnp.sqrt(frob + EPS)

        def refresh(block):
            at, here = unit_rows(block), block_rows(block)
            update = weights[m, at, :].astype(F32) - scale * whole[m, here, :].astype(F32)
            length = jnp.sqrt(jnp.sum(update * update, axis=-1, keepdims=True) + EPS)
            weights[m, at, :] = (update * (target[m, here, :] / length)).astype(BF16)

        each(half // BLOCK, refresh, half // BLOCK)

    def share_memory(m):
        at = weights.at[m, own_units]
        return remote(at, at, w_sem.at[0, m], w_sem.at[1, m], partner)

    def all_tokens(s, g):
        return feat[s, g, :parcel].reshape(everyone, width)

    def read_copy(g, b):
        there, row = readers(b)
        return remote(ro_send.at[g, b], out_ref.at[g, head * PAIR + col],
                      ro_sem.at[0, g, b], ro_sem.at[1, g, b], device(line, there, core, row))

    def read_block(g, b):
        there, row = readers(b)
        queries = feat[0, g, there * CORES + core, pl.ds(pl.multiple_of(row * quarter, BLOCK), quarter), :]
        hidden, gated = dot_nt(queries, weights[0]), dot_nt(queries, weights[1])
        readmix = (hidden * jax.nn.sigmoid(hidden) * gated).astype(BF16)
        return dot(readmix, weights[2]).astype(BF16)

    def read_ship(g, b):
        ro_send[g, b] = read_block(g, b)
        read_copy(g, b).start()

    def read_keep(g):
        out_ref[g, head * PAIR + col] = read_block(g, last_block)

    def read_ready(g):
        for m in range(3):
            share_memory(m).wait()
        for h in range(HALVES):
            across_copy(g, 0, h).wait()

    stages = (2, 1, 0)

    def inner_step(g, step):
        keys, signal = all_tokens(1, g), all_tokens(2, g)
        own_first, own_third, own_second = (weights[m, own_units, :] for m in range(3))
        hid[...] = dot_nt(own_first, keys)
        gat[...] = dot_nt(own_third, keys)
        bak[...] = dot_nt(own_second, signal)
        strips = 4
        strip = everyone // strips

        def pointwise(i):
            at = block_rows(i // strips), pl.ds(pl.multiple_of((i % strips) * strip, LANES), strip)
            hidden, gated, back = hid[at], gat[at], bak[at]
            sigma = jax.nn.sigmoid(hidden)
            act = hidden * sigma
            mixed[at] = (act * gated).astype(BF16)
            dgate[at] = (back * act).astype(BF16)
            dfirst[at] = (back * gated * (sigma * (1.0 + hidden * (1.0 - sigma)))).astype(BF16)

        each(half // BLOCK * strips, pointwise, strips)
        factors = {2: (mixed, signal), 1: (dgate, keys), 0: (dfirst, keys)}
        for m in stages:
            left, right = factors[m]
            grads[m] = dot(left[...], right).astype(BF16)
            for k in range(PARTS):
                launch(step, m, k)

        chunks = [(m, k) for m in stages for k in range(PARTS)]
        skew, lag = 3, 2
        for turn in range(len(chunks) + skew + lag):
            if turn < len(chunks):
                relay(step, *chunks[turn])
            if 0 <= turn - skew < len(chunks):
                m, k = chunks[turn - skew]
                finish(step, m, k)
                if k == PARTS - 1:
                    measure(step, m)
            if 0 <= turn - skew - lag < len(chunks):
                m, k = chunks[turn - skew - lag]
                if k == PARTS - 1:
                    update_memory(step, m)
                    if step == INNER - 1:
                        share_memory(m).start()
            if step == 0 and turn == 0:
                @pl.when(g > 0)
                def _():
                    read_ready(g - 1)
            if step == 0 and turn < last_block:
                @pl.when(g > 0)
                def _(turn=turn):
                    read_ship(g - 1, turn)
            if step == 0 and turn == last_block:
                @pl.when(g > 0)
                def _():
                    read_keep(g - 1)
            if step == INNER - 1 and turn == 0:
                for h in range(HALVES):
                    across_copy(g, 0, h).start()
            if step == INNER - 1 and turn == 5:
                @pl.when(g < groups - 1)
                def _():
                    pass_on(g + 1)
        for m in stages:
            drain(step, m)

    def group(g):
        settle(g)

        @pl.when(g > 0)
        def _():
            for h in range(HALVES):
                for s in (1, 2):
                    across_copy(g, s, h).wait_send()

        for step in range(INNER):
            inner_step(g, step)

    each(groups, group)
    read_ready(groups - 1)
    each(last_block, lambda b: read_ship(groups - 1, b))
    read_keep(groups - 1)

    def land(i):
        read_copy(i // last_block, i % last_block).wait()

    each(groups * last_block, land)


def normalize_kernel(parts_ref, gain_ref, out_ref):
    heads, rows, width = parts_ref.shape[1:]
    for block in range(rows // BLOCK):
        at = slice(block * BLOCK, (block + 1) * BLOCK)
        parts = [parts_ref[0, i, at, :].astype(F32) for i in range(heads)]
        square = jnp.sum(sum(part * part for part in parts), axis=-1, keepdims=True)
        factor = lax.rsqrt(square / (heads * width) + EPS)
        for i, part in enumerate(parts):
            columns = slice(i * width, (i + 1) * width)
            out_ref[0, at, columns] = (part * factor * gain_ref[:, columns]).astype(BF16)


def solution(mesh):
    tok_size, head_size = mesh.shape["tok"], mesh.shape["head"]

    def body(inputs, projections, lrate, fast_init, gain):
        groups, tokens, depth = inputs.shape
        heads, _, units, width = fast_init.shape
        assert heads == PAIR and INNER == 2
        half = units // CORES
        everyone = PAIR * CORES * tokens
        quarter = tokens // head_size
        all_heads = PAIR * head_size
        parts = pl.pallas_call(
            functools.partial(train_kernel, tok_size, head_size),
            out_shape=jax.ShapeDtypeStruct((groups, all_heads, quarter, width), BF16),
            in_specs=[
                pl.BlockSpec(memory_space=pl.ANY),
                pl.BlockSpec(memory_space=pl.ANY),
                pl.BlockSpec(memory_space=pltpu.VMEM),
                pl.BlockSpec(memory_space=pl.ANY),
            ],
            out_specs=pl.BlockSpec(memory_space=pltpu.VMEM),
            scratch_shapes=[
                pltpu.VMEM((groups, tokens, depth), BF16),
                pltpu.VMEM((3, 2, depth, width), BF16),
                pltpu.VMEM((groups, 2, tokens, LANES), F32),
                pltpu.VMEM((3, groups, PAIR * CORES + 1, tokens, width), BF16),
                pltpu.VMEM((3, units, width), BF16),
                pltpu.VMEM((3, half, 1), F32),
                pltpu.VMEM((half, everyone), F32),
                pltpu.VMEM((half, everyone), F32),
                pltpu.VMEM((half, everyone), F32),
                pltpu.VMEM((half, everyone), BF16),
                pltpu.VMEM((half, everyone), BF16),
                pltpu.VMEM((half, everyone), BF16),
                pltpu.VMEM((3, half, width), BF16),
                pltpu.VMEM((3, half, width), BF16),
                pltpu.VMEM((3, half, width), BF16),
                pltpu.VMEM((INNER, 3, half, width), BF16),
                pltpu.VMEM((3, half, width), BF16),
                pltpu.VMEM((INNER, 2, 3, 8, LANES), F32),
                pltpu.VMEM((groups, all_heads - 1, quarter, width), BF16),
                pltpu.SemaphoreType.DMA((7 + groups,)),
                pltpu.SemaphoreType.DMA((2, 3, groups, HALVES)),
                pltpu.SemaphoreType.DMA((2, 3, groups, HALVES)),
                pltpu.SemaphoreType.DMA((2, 3, groups, HALVES)),
                pltpu.SemaphoreType.DMA((8 + INNER, 3, PARTS)),
                pltpu.SemaphoreType.DMA((2, 3)),
                pltpu.SemaphoreType.DMA((2, groups, all_heads - 1)),
            ],
            compiler_params=pltpu.CompilerParams(
                collective_id=0, has_side_effects=True, vmem_limit_bytes=60000 * 1024
            ),
        )(inputs, projections, lrate.transpose(0, 2, 1), fast_init)
        return pl.pallas_call(
            normalize_kernel,
            grid=(groups, quarter // NORM_ROWS),
            out_shape=jax.ShapeDtypeStruct((groups, quarter, all_heads * width), BF16),
            in_specs=[
                pl.BlockSpec((1, all_heads, NORM_ROWS, width), lambda g, i: (g, 0, i, 0)),
                pl.BlockSpec((1, all_heads * width), lambda g, i: (0, 0)),
            ],
            out_specs=pl.BlockSpec((1, NORM_ROWS, all_heads * width), lambda g, i: (g, i, 0)),
        )(parts, gain[None])

    return jax.shard_map(
        body,
        mesh=mesh,
        in_specs=(
            P(None, "tok", None),
            P(None, None, "head"),
            P(None, "tok", "head"),
            P("head", None, None, None),
            P(),
        ),
        out_specs=P(None, ("tok", "head"), None),
        check_vma=False,
    )
```

```python
import functools

import jax
import jax.numpy as jnp
from jax import lax
from jax.experimental import pallas as pl
from jax.experimental.pallas import tpu as pltpu
from jax.sharding import PartitionSpec as P

INNER = 2
CORES = 2
PAIR = 2
PARTS = 4
HALVES = 2
STEP_SIZE = 4.0
EPS = 1e-06
MESH = pl.DeviceIdType.MESH
BLOCK = 16
LANES = 128
NORM_ROWS = 256
SKEW = 3
LAG = 2
NT = (((1,), (1,)), ((), ()))
F32, BF16 = jnp.float32, jnp.bfloat16


def dot(left, right):
    return jnp.dot(left, right, preferred_element_type=F32)


def dot_nt(left, right):
    return lax.dot_general(left, right, NT, preferred_element_type=F32)


def train_kernel(
    tok_size, head_size,
    x_hbm, w_hbm, lr_ref, init_hbm, out_ref,
    x, w, rate, feat, weights, target, hid, gat, bak, mixed, dgate, dfirst,
    grads, in_recv, partial, mid_recv, whole, sumsq, ro_send,
    load_sem, x_sem, own_sem, fwd_sem, red_sem, w_sem, ro_sem,
):
    groups, tokens, depth = x.shape
    units, width = weights.shape[1], weights.shape[2]
    half = units // CORES
    piece = half // PARTS
    everyone = PAIR * CORES * tokens
    stripe = tokens // HALVES
    quarter = tokens // head_size
    lines = tok_size // (CORES * PAIR)
    reach = lines // 2

    tok, head = lax.axis_index("tok"), lax.axis_index("head")
    core, chip = tok % CORES, tok // CORES
    col, line = chip % PAIR, chip // PAIR
    low = line < reach
    pos = jnp.where(low, line, lines - 1 - line)
    inward = jnp.where(low, 1, -1)
    center, end = pos == reach - 1, pos == 0

    def device(line_, col_, core_, head_):
        return {"tok": (line_ * PAIR + col_) * CORES + core_, "head": head_}

    partner = device(line, col, 1 - core, head)
    across = device(line, 1 - col, core, head)
    inner = device(line + inward, col, core, head)
    outer = device((line - inward + lines) % lines, col, core, head)

    def readers(b):
        dx, dy = 1 - b // head_size, head_size - 1 - b % head_size
        return (col + dx) % PAIR, (head + dy) % head_size

    last_block = PAIR * head_size - 1

    def remote(source, destination, send, recv, to):
        return pltpu.make_async_remote_copy(
            src_ref=source, dst_ref=destination, send_sem=send, recv_sem=recv, device_id=to, device_id_type=MESH
        )

    loads = [pltpu.make_async_copy(x_hbm.at[0], x.at[0], load_sem.at[0])]
    order = [(1, 0), (2, 0), (1, 1), (2, 1), (0, 0), (0, 1)]
    for i, (s, own) in enumerate(order):
        start = pl.multiple_of((col if own else 1 - col) * width, LANES)
        loads.append(pltpu.make_async_copy(
            w_hbm.at[s, :, pl.ds(start, width)], w.at[s, own], load_sem.at[1 + i]))
    for g in range(1, groups):
        loads.append(pltpu.make_async_copy(x_hbm.at[g], x.at[g], load_sem.at[7 + g]))
    own_units = pl.ds(pl.multiple_of(core * half, BLOCK), half)
    load_init = pltpu.make_async_copy(
        init_hbm.at[col, :, own_units], weights.at[:, own_units], load_sem.at[7])
    for copy in loads[:5] + [load_init] + loads[5:]:
        copy.start()

    barrier = pltpu.get_barrier_semaphore()
    pl.semaphore_signal(barrier, inc=1, device_id=partner, device_id_type=MESH)
    pl.semaphore_signal(barrier, inc=1, device_id=inner, device_id_type=MESH)
    for b in range(last_block):
        there, row = readers(b)
        pl.semaphore_signal(barrier, inc=1, device_id=device(line, there, core, row), device_id_type=MESH)
    pl.semaphore_signal(barrier, inc=1, device_id=outer, device_id_type=MESH)

    for g in range(groups):
        for own in range(2):
            which = col if own else 1 - col
            row = lr_ref[g, pl.ds(which, 1), :]
            rate[g, own] = -jnp.transpose(jnp.broadcast_to(row, (LANES, tokens)))

    def stripe_rows(h):
        return pl.ds(pl.multiple_of(h * stripe, stripe), stripe)

    mine, theirs = col * CORES + core, (1 - col) * CORES + core
    parcel = PAIR * CORES

    def project(g, s, own, h):
        rows = stripe_rows(h)
        got = dot(x[g, rows, :], w[s, own]).astype(BF16).astype(F32)
        factor = jnp.where(s == 2, rate[g, own, rows, :], 1.0)
        slot = mine if own else parcel
        for j in range(width // LANES):
            columns = slice(j * LANES, (j + 1) * LANES)
            feat[s, g, slot, rows, columns] = (got[:, columns] * factor).astype(BF16)

    def across_copy(g, s, h):
        rows = stripe_rows(h)
        return remote(feat.at[s, g, parcel, rows], feat.at[s, g, mine, rows],
                      x_sem.at[0, s, g, h], x_sem.at[1, s, g, h], across)

    def own_copy(g, s, h):
        at = feat.at[s, g, mine, stripe_rows(h)]
        return remote(at, at, own_sem.at[0, s, g, h], own_sem.at[1, s, g, h], partner)

    def forward_copy(g, s, h):
        at = feat.at[s, g, theirs, stripe_rows(h)]
        return remote(at, at, fwd_sem.at[0, s, g, h], fwd_sem.at[1, s, g, h], partner)

    def each(count, work, unroll=1):
        def one(i, carry):
            work(i)
            return carry

        lax.fori_loop(0, count, one, 0, unroll=unroll)

    pl.semaphore_wait(barrier, 3 + last_block)
    for copy in loads[:3]:
        copy.wait()

    def ship_first(i):
        s, h = 1 + i % 2, i // 2
        project(0, s, 0, h)
        across_copy(0, s, h).start()

    each(2 * HALVES, ship_first)
    for copy in loads[3:5]:
        copy.wait()

    def keep_first(i):
        s, h = 1 + i % 2, i // 2
        project(0, s, 1, h)
        own_copy(0, s, h).start()

    each(2 * HALVES, keep_first)
    load_init.wait()

    def unit_rows(block):
        return pl.ds(pl.multiple_of(core * half + block * BLOCK, BLOCK), BLOCK)

    def block_rows(block):
        return pl.ds(pl.multiple_of(block * BLOCK, BLOCK), BLOCK)

    def prepare(i):
        m, block = i // (half // BLOCK), i % (half // BLOCK)
        start = weights[m, unit_rows(block), :].astype(F32)
        target[m, block_rows(block), :] = jnp.sqrt(jnp.sum(start * start, axis=-1, keepdims=True))

    each(3 * half // BLOCK, prepare, half // BLOCK)
    for copy in loads[5:]:
        copy.wait()

    def ship_rest(i):
        g, j = 1 + i // (2 * HALVES), i % (2 * HALVES)
        project(g, 1 + j % 2, 0, j // 2)

    each((groups - 1) * 2 * HALVES, ship_rest)

    def keep_rest(i):
        g, j = 1 + i // (2 * HALVES), i % (2 * HALVES)
        s, h = 1 + j % 2, j // 2
        project(g, s, 1, h)
        own_copy(g, s, h).start()

    each((groups - 1) * 2 * HALVES, keep_rest)

    def read_other(i):
        project(i // HALVES, 0, 0, i % HALVES)

    def read_own(i):
        project(i // HALVES, 0, 1, i % HALVES)

    each(groups * HALVES, read_other)
    each(groups * HALVES, read_own)

    def pass_on(g):
        for h in range(HALVES):
            for s in (1, 2):
                across_copy(g, s, h).wait_recv()
                forward_copy(g, s, h).start()

    def settle(g):
        for h in range(HALVES):
            for s in (1, 2):
                own_copy(g, s, h).wait()
                forward_copy(g, s, h).wait()

    pass_on(0)
    for h in range(HALVES):
        for s in (1, 2):
            across_copy(0, s, h).wait_send()
    for g in range(1, groups):
        for h in range(HALVES):
            for s in (1, 2):
                across_copy(g, s, h).start()

    def chunk_rows(k):
        return slice(k * piece, (k + 1) * piece)

    def send_in(step, m, k, source):
        at = chunk_rows(k)
        return remote(source.at[step, m, at], in_recv.at[step, m, at],
                      red_sem.at[0, step, m, k], red_sem.at[1, step, m, k], inner)

    def send_mid(step, m, k):
        at = chunk_rows(k)
        source = grads if reach == 1 else partial
        return remote(source.at[step, m, at], mid_recv.at[step, m, at],
                      red_sem.at[2, step, m, k], red_sem.at[3, step, m, k], inner)

    def send_out(step, m, k):
        at = whole.at[step, m, chunk_rows(k)]
        return remote(at, at, red_sem.at[4, step, m, k], red_sem.at[5, step, m, k], outer)

    def launch(step, m):
        @pl.when(end)
        def _():
            for k in range(PARTS):
                if reach == 1:
                    send_mid(step, m, k).start()
                else:
                    send_in(step, m, k, grads).start()

    def relay(step, m, k):
        @pl.when(pos > 0)
        def _():
            at = chunk_rows(k)
            send_in(step, m, k, grads).wait_recv()
            total = grads[step, m, at, :].astype(F32) + in_recv[step, m, at, :].astype(F32)
            partial[step, m, at, :] = total.astype(BF16)

            @pl.when(center)
            def _():
                send_mid(step, m, k).start()

            if reach > 2:
                @pl.when(jnp.logical_not(center))
                def _():
                    send_in(step, m, k, partial).start()

    def finish(step, m, k):
        @pl.when(center)
        def _():
            at = chunk_rows(k)
            send_mid(step, m, k).wait_recv()
            source = grads if reach == 1 else partial
            total = source[step, m, at, :].astype(F32) + mid_recv[step, m, at, :].astype(F32)
            whole[step, m, at, :] = total.astype(BF16)
            if reach > 1:
                send_out(step, m, k).start()

    def collect(step, m):
        if reach > 1:
            @pl.when(jnp.logical_not(center))
            def _():
                for k in range(PARTS):
                    send_out(step, m, k).wait_recv()
                    if reach > 2:
                        @pl.when(pos > 0)
                        def _(k=k):
                            send_out(step, m, k).start()

    def drain(step, m):
        for k in range(PARTS):
            @pl.when(center)
            def _(k=k):
                send_mid(step, m, k).wait_send()

            if reach > 1:
                @pl.when(jnp.logical_not(center))
                def _(k=k):
                    send_in(step, m, k, grads).wait_send()

                @pl.when(pos > 0)
                def _(k=k):
                    send_out(step, m, k).wait_send()

    def share_square(step, m):
        return remote(sumsq.at[step, 0, m], sumsq.at[step, 1, m],
                      red_sem.at[6, step, m, 0], red_sem.at[7, step, m, 0], partner)

    def measure(step, m):
        collect(step, m)
        total = jnp.zeros((BLOCK, width), F32)
        for block in range(half // BLOCK):
            part = whole[step, m, block * BLOCK:(block + 1) * BLOCK, :].astype(F32)
            total = total + part * part
        total = total[:8] + total[8:]
        sumsq[step, 0, m] = sum(total[:, j * LANES:(j + 1) * LANES] for j in range(width // LANES))
        share_square(step, m).start()

    def update_memory(step, m):
        share_square(step, m).wait()
        both = sumsq[step, 0, m] + sumsq[step, 1, m]
        frob = jnp.sum(jnp.sum(both, axis=0, keepdims=True), axis=1, keepdims=True)
        scale = STEP_SIZE / jnp.sqrt(frob + EPS)

        def refresh(block):
            at, here = unit_rows(block), block_rows(block)
            update = weights[m, at, :].astype(F32) - scale * whole[step, m, here, :].astype(F32)
            length = jnp.sqrt(jnp.sum(update * update, axis=-1, keepdims=True) + EPS)
            weights[m, at, :] = (update * (target[m, here, :] / length)).astype(BF16)

        each(half // BLOCK, refresh, half // BLOCK)

    def share_memory(m):
        at = weights.at[m, own_units]
        return remote(at, at, w_sem.at[0, m], w_sem.at[1, m], partner)

    def all_tokens(s, g):
        return feat[s, g, :parcel].reshape(everyone, width)

    def read_copy(g, b):
        there, row = readers(b)
        return remote(ro_send.at[g, b], out_ref.at[g, head * PAIR + col],
                      ro_sem.at[0, g, b], ro_sem.at[1, g, b], device(line, there, core, row))

    def read_block(g, b):
        there, row = readers(b)
        queries = feat[0, g, there * CORES + core, pl.ds(pl.multiple_of(row * quarter, BLOCK), quarter), :]
        hidden, gated = dot_nt(queries, weights[0]), dot_nt(queries, weights[1])
        readmix = (hidden * jax.nn.sigmoid(hidden) * gated).astype(BF16)
        return dot(readmix, weights[2]).astype(BF16)

    def read_ship(g, b):
        ro_send[g, b] = read_block(g, b)
        read_copy(g, b).start()

    def read_keep(g):
        out_ref[g, head * PAIR + col] = read_block(g, last_block)

    def read_ready(g):
        for m in range(3):
            share_memory(m).wait()
        for h in range(HALVES):
            across_copy(g, 0, h).wait()

    strips = 4
    strip = everyone // strips

    def strips_of(i):
        return block_rows(i // strips), pl.ds(pl.multiple_of((i % strips) * strip, LANES), strip)

    def pointwise_first(i):
        at = strips_of(i)
        hidden, gated = hid[at], gat[at]
        sigma = jax.nn.sigmoid(hidden)
        act = hidden * sigma
        mixed[at] = (act * gated).astype(BF16)
        hid[at] = act
        gat[at] = gated * (sigma * (1.0 + hidden * (1.0 - sigma)))

    def pointwise_last(i):
        at = strips_of(i)
        back = bak[at]
        dgate[at] = (back * hid[at]).astype(BF16)
        dfirst[at] = (back * gat[at]).astype(BF16)

    def over_tokens(work):
        each(half // BLOCK * strips, work, strips)

    def group(g):
        settle(g)

        @pl.when(g > 0)
        def _():
            for h in range(HALVES):
                for s in (1, 2):
                    across_copy(g, s, h).wait_send()

        def look():
            pair = weights[0:2, own_units, :].reshape(2 * half, width)
            both = dot_nt(pair, all_tokens(1, g))
            hid[...] = both[:half]
            gat[...] = both[half:]

        def look_back():
            bak[...] = dot_nt(weights[2, own_units, :], all_tokens(2, g))

        def gradient(step, m):
            left, s = ((dfirst, 1), (dgate, 1), (mixed, 2))[m]
            grads[step, m] = dot(left[...], all_tokens(s, g)).astype(BF16)
            launch(step, m)

        orders = ((0, 1, 2), (2, 0, 1))
        chunks = [(step, m, k) for step in range(INNER) for m in orders[step] for k in range(PARTS)]
        per_step = 3 * PARTS

        def relay_at(q):
            relay(*chunks[q])

        def finish_at(q):
            finish(*chunks[q])

        def pass_turn(turn, first, last):
            if turn < last:
                relay_at(turn)
            q = turn - SKEW
            if first <= q < last:
                finish_at(q)
                step, m, k = chunks[q]
                if k == PARTS - 1:
                    measure(step, m)
            if first <= q - LAG < last:
                step, m, k = chunks[q - LAG]
                if k == PARTS - 1:
                    update_memory(step, m)
                    if step == INNER - 1:
                        share_memory(m).start()

        look()
        over_tokens(pointwise_first)
        look_back()
        over_tokens(pointwise_last)
        for m in orders[0]:
            gradient(0, m)

        for turn in range(per_step):
            pass_turn(turn, 0, per_step)
            if turn == 0:
                @pl.when(g > 0)
                def _():
                    read_ready(g - 1)
            if turn <= last_block:
                @pl.when(g > 0)
                def _(turn=turn):
                    if turn < last_block:
                        read_ship(g - 1, turn)
                    else:
                        read_keep(g - 1)
        update_memory(0, 1)
        look()
        finish_at(per_step - 3)
        over_tokens(pointwise_first)
        finish_at(per_step - 2)
        gradient(1, 2)
        finish_at(per_step - 1)
        measure(0, 2)
        for h in range(HALVES):
            across_copy(g, 0, h).start()
        update_memory(0, 2)
        look_back()
        relay_at(per_step)
        over_tokens(pointwise_last)
        relay_at(per_step + 1)
        gradient(1, 0)
        relay_at(per_step + 2)
        gradient(1, 1)
        for turn in range(per_step + SKEW, 2 * per_step + SKEW + LAG):
            pass_turn(turn, per_step, 2 * per_step)
            if turn == per_step + 7:
                @pl.when(g < groups - 1)
                def _():
                    pass_on(g + 1)
        for step in range(INNER):
            for m in range(3):
                drain(step, m)

    each(groups, group)
    read_ready(groups - 1)
    each(last_block, lambda b: read_ship(groups - 1, b))
    read_keep(groups - 1)

    def land(i):
        read_copy(i // last_block, i % last_block).wait()

    each(groups * last_block, land)


def normalize_kernel(parts_ref, gain_ref, out_ref):
    heads, rows, width = parts_ref.shape[1:]
    for block in range(rows // BLOCK):
        at = slice(block * BLOCK, (block + 1) * BLOCK)
        parts = [parts_ref[0, i, at, :].astype(F32) for i in range(heads)]
        square = jnp.sum(sum(part * part for part in parts), axis=-1, keepdims=True)
        factor = lax.rsqrt(square / (heads * width) + EPS)
        for i, part in enumerate(parts):
            columns = slice(i * width, (i + 1) * width)
            out_ref[0, at, columns] = (part * factor * gain_ref[:, columns]).astype(BF16)


def solution(mesh):
    tok_size, head_size = mesh.shape["tok"], mesh.shape["head"]

    def body(inputs, projections, lrate, fast_init, gain):
        groups, tokens, depth = inputs.shape
        heads, _, units, width = fast_init.shape
        assert heads == PAIR and INNER == 2
        half = units // CORES
        everyone = PAIR * CORES * tokens
        quarter = tokens // head_size
        all_heads = PAIR * head_size
        parts = pl.pallas_call(
            functools.partial(train_kernel, tok_size, head_size),
            out_shape=jax.ShapeDtypeStruct((groups, all_heads, quarter, width), BF16),
            in_specs=[
                pl.BlockSpec(memory_space=pl.ANY),
                pl.BlockSpec(memory_space=pl.ANY),
                pl.BlockSpec(memory_space=pltpu.VMEM),
                pl.BlockSpec(memory_space=pl.ANY),
            ],
            out_specs=pl.BlockSpec(memory_space=pltpu.VMEM),
            scratch_shapes=[
                pltpu.VMEM((groups, tokens, depth), BF16),
                pltpu.VMEM((3, 2, depth, width), BF16),
                pltpu.VMEM((groups, 2, tokens, LANES), F32),
                pltpu.VMEM((3, groups, PAIR * CORES + 1, tokens, width), BF16),
                pltpu.VMEM((3, units, width), BF16),
                pltpu.VMEM((3, half, 1), F32),
                pltpu.VMEM((half, everyone), F32),
                pltpu.VMEM((half, everyone), F32),
                pltpu.VMEM((half, everyone), F32),
                pltpu.VMEM((half, everyone), BF16),
                pltpu.VMEM((half, everyone), BF16),
                pltpu.VMEM((half, everyone), BF16),
                pltpu.VMEM((INNER, 3, half, width), BF16),
                pltpu.VMEM((INNER, 3, half, width), BF16),
                pltpu.VMEM((INNER, 3, half, width), BF16),
                pltpu.VMEM((INNER, 3, half, width), BF16),
                pltpu.VMEM((INNER, 3, half, width), BF16),
                pltpu.VMEM((INNER, 2, 3, 8, LANES), F32),
                pltpu.VMEM((groups, all_heads - 1, quarter, width), BF16),
                pltpu.SemaphoreType.DMA((7 + groups,)),
                pltpu.SemaphoreType.DMA((2, 3, groups, HALVES)),
                pltpu.SemaphoreType.DMA((2, 3, groups, HALVES)),
                pltpu.SemaphoreType.DMA((2, 3, groups, HALVES)),
                pltpu.SemaphoreType.DMA((8, INNER, 3, PARTS)),
                pltpu.SemaphoreType.DMA((2, 3)),
                pltpu.SemaphoreType.DMA((2, groups, all_heads - 1)),
            ],
            compiler_params=pltpu.CompilerParams(
                collective_id=0, has_side_effects=True, vmem_limit_bytes=60000 * 1024
            ),
        )(inputs, projections, lrate.transpose(0, 2, 1), fast_init)
        return pl.pallas_call(
            normalize_kernel,
            grid=(groups, quarter // NORM_ROWS),
            out_shape=jax.ShapeDtypeStruct((groups, quarter, all_heads * width), BF16),
            in_specs=[
                pl.BlockSpec((1, all_heads, NORM_ROWS, width), lambda g, i: (g, 0, i, 0)),
                pl.BlockSpec((1, all_heads * width), lambda g, i: (0, 0)),
            ],
            out_specs=pl.BlockSpec((1, NORM_ROWS, all_heads * width), lambda g, i: (g, i, 0)),
        )(parts, gain[None])

    return jax.shard_map(
        body,
        mesh=mesh,
        in_specs=(
            P(None, "tok", None),
            P(None, None, "head"),
            P(None, "tok", "head"),
            P("head", None, None, None),
            P(),
        ),
        out_specs=P(None, ("tok", "head"), None),
        check_vma=False,
    )
```

```python
import functools

import jax
import jax.numpy as jnp
from jax import lax
from jax.experimental import pallas as pl
from jax.experimental.pallas import tpu as pltpu
from jax.sharding import PartitionSpec as P

INNER = 2
CORES = 2
PAIR = 2
CUTS = (0, 3, 6, 9, 12)
PARTS = len(CUTS) - 1
HALVES = 2
STEP_SIZE = 4.0
EPS = 1e-06
MESH = pl.DeviceIdType.MESH
BLOCK = 16
LANES = 128
NORM_ROWS = 256
SKEW = 3
LAG = 2
NT = (((1,), (1,)), ((), ()))
F32, BF16 = jnp.float32, jnp.bfloat16


def dot(left, right):
    return jnp.dot(left, right, preferred_element_type=F32)


def dot_nt(left, right):
    return lax.dot_general(left, right, NT, preferred_element_type=F32)


def train_kernel(
    tok_size, head_size,
    x_hbm, w_hbm, lr_ref, init_hbm, out_ref,
    x, w, rate, feat, weights, target, hid, gat, bak, mixed, dgate, dfirst,
    grads, in_recv, partial, mid_recv, whole, sumsq, ro_send,
    load_sem, x_sem, own_sem, fwd_sem, red_sem, w_sem, ro_sem,
):
    groups, tokens, depth = x.shape
    units, width = weights.shape[1], weights.shape[2]
    half = units // CORES
    piece = half // CUTS[-1]
    everyone = PAIR * CORES * tokens
    stripe = tokens // HALVES
    quarter = tokens // head_size
    lines = tok_size // (CORES * PAIR)
    reach = lines // 2

    tok, head = lax.axis_index("tok"), lax.axis_index("head")
    core, chip = tok % CORES, tok // CORES
    col, line = chip % PAIR, chip // PAIR
    low = line < reach
    pos = jnp.where(low, line, lines - 1 - line)
    inward = jnp.where(low, 1, -1)
    center, end = pos == reach - 1, pos == 0

    def device(line_, col_, core_, head_):
        return {"tok": (line_ * PAIR + col_) * CORES + core_, "head": head_}

    partner = device(line, col, 1 - core, head)
    across = device(line, 1 - col, core, head)
    inner = device(line + inward, col, core, head)
    outer = device((line - inward + lines) % lines, col, core, head)

    def readers(b):
        dx, dy = 1 - b // head_size, head_size - 1 - b % head_size
        return (col + dx) % PAIR, (head + dy) % head_size

    last_block = PAIR * head_size - 1

    def remote(source, destination, send, recv, to):
        return pltpu.make_async_remote_copy(
            src_ref=source, dst_ref=destination, send_sem=send, recv_sem=recv, device_id=to, device_id_type=MESH
        )

    loads = [pltpu.make_async_copy(x_hbm.at[0], x.at[0], load_sem.at[0])]
    order = [(2, 0), (1, 0), (2, 1), (1, 1), (0, 0), (0, 1)]
    for i, (s, own) in enumerate(order):
        start = pl.multiple_of((col if own else 1 - col) * width, LANES)
        loads.append(pltpu.make_async_copy(
            w_hbm.at[s, :, pl.ds(start, width)], w.at[s, own], load_sem.at[1 + i]))
    for g in range(1, groups):
        loads.append(pltpu.make_async_copy(x_hbm.at[g], x.at[g], load_sem.at[7 + g]))
    own_units = pl.ds(pl.multiple_of(core * half, BLOCK), half)
    load_init = pltpu.make_async_copy(
        init_hbm.at[col, :, own_units], weights.at[:, own_units], load_sem.at[7])
    for copy in loads[:5] + [load_init] + loads[5:]:
        copy.start()

    barrier = pltpu.get_barrier_semaphore()
    pl.semaphore_signal(barrier, inc=1, device_id=partner, device_id_type=MESH)
    pl.semaphore_signal(barrier, inc=1, device_id=inner, device_id_type=MESH)
    for b in range(last_block):
        there, row = readers(b)
        pl.semaphore_signal(barrier, inc=1, device_id=device(line, there, core, row), device_id_type=MESH)
    pl.semaphore_signal(barrier, inc=1, device_id=outer, device_id_type=MESH)

    for g in range(groups):
        for own in range(2):
            which = col if own else 1 - col
            row = lr_ref[g, pl.ds(which, 1), :]
            rate[g, own] = -jnp.transpose(jnp.broadcast_to(row, (LANES, tokens)))

    def stripe_rows(h):
        return pl.ds(pl.multiple_of(h * stripe, stripe), stripe)

    mine, theirs = col * CORES + core, (1 - col) * CORES + core
    parcel = PAIR * CORES

    def project(g, s, own, h):
        rows = stripe_rows(h)
        got = dot(x[g, rows, :], w[s, own]).astype(BF16).astype(F32)
        factor = jnp.where(s == 2, rate[g, own, rows, :], 1.0)
        slot = mine if own else parcel
        for j in range(width // LANES):
            columns = slice(j * LANES, (j + 1) * LANES)
            feat[s, g, slot, rows, columns] = (got[:, columns] * factor).astype(BF16)

    def across_copy(g, s, h):
        rows = stripe_rows(h)
        return remote(feat.at[s, g, parcel, rows], feat.at[s, g, mine, rows],
                      x_sem.at[0, s, g, h], x_sem.at[1, s, g, h], across)

    def own_copy(g, s, h):
        at = feat.at[s, g, mine, stripe_rows(h)]
        return remote(at, at, own_sem.at[0, s, g, h], own_sem.at[1, s, g, h], partner)

    def forward_copy(g, s, h):
        at = feat.at[s, g, theirs, stripe_rows(h)]
        return remote(at, at, fwd_sem.at[0, s, g, h], fwd_sem.at[1, s, g, h], partner)

    def each(count, work, unroll=1):
        def one(i, carry):
            work(i)
            return carry

        lax.fori_loop(0, count, one, 0, unroll=unroll)

    pl.semaphore_wait(barrier, 3 + last_block)
    loads[0].wait()
    for s in (2, 1):
        loads[3 - s].wait()

        def ship_first(h, s=s):
            project(0, s, 0, h)
            across_copy(0, s, h).start()

        each(HALVES, ship_first)

    for copy in loads[3:5]:
        copy.wait()

    def keep_first(i):
        s, h = 2 - i // HALVES, i % HALVES
        project(0, s, 1, h)
        own_copy(0, s, h).start()

    each(2 * HALVES, keep_first)
    load_init.wait()

    def unit_rows(block):
        return pl.ds(pl.multiple_of(core * half + block * BLOCK, BLOCK), BLOCK)

    def block_rows(block):
        return pl.ds(pl.multiple_of(block * BLOCK, BLOCK), BLOCK)

    def prepare(i):
        m, block = i // (half // BLOCK), i % (half // BLOCK)
        start = weights[m, unit_rows(block), :].astype(F32)
        target[m, block_rows(block), :] = jnp.sqrt(jnp.sum(start * start, axis=-1, keepdims=True))

    each(3 * half // BLOCK, prepare, half // BLOCK)
    for copy in loads[5:]:
        copy.wait()

    def ship_rest(i):
        g, j = 1 + i // (2 * HALVES), i % (2 * HALVES)
        project(g, 1 + j % 2, 0, j // 2)

    each((groups - 1) * 2 * HALVES, ship_rest)

    def keep_rest(i):
        g, j = 1 + i // (2 * HALVES), i % (2 * HALVES)
        s, h = 1 + j % 2, j // 2
        project(g, s, 1, h)
        own_copy(g, s, h).start()

    each((groups - 1) * 2 * HALVES, keep_rest)

    def read_other(i):
        project(i // HALVES, 0, 0, i % HALVES)

    def read_own(i):
        project(i // HALVES, 0, 1, i % HALVES)

    each(groups * HALVES, read_other)
    each(groups * HALVES, read_own)

    def pass_on(g):
        for s in (2, 1):
            for h in range(HALVES):
                pass_piece(g, s, h)

    def pass_piece(g, s, h):
        across_copy(g, s, h).wait_recv()
        forward_copy(g, s, h).start()

    def settle(g, s):
        for h in range(HALVES):
            own_copy(g, s, h).wait()
            forward_copy(g, s, h).wait()

    def all_tokens(s, g):
        return feat[s, g, :parcel].reshape(everyone, width)

    def look_back(g):
        settle(g, 2)
        bak[...] = dot_nt(weights[2, own_units, :], all_tokens(2, g))

    for h in range(HALVES):
        pass_piece(0, 2, h)
    for h in range(HALVES - 1):
        pass_piece(0, 1, h)
    look_back(0)
    pass_piece(0, 1, HALVES - 1)
    for h in range(HALVES):
        for s in (1, 2):
            across_copy(0, s, h).wait_send()
    for g in range(1, groups):
        for s in (2, 1):
            for h in range(HALVES):
                across_copy(g, s, h).start()

    def chunk_rows(k):
        return slice(CUTS[k] * piece, CUTS[k + 1] * piece)

    def send_in(step, m, k, source):
        at = chunk_rows(k)
        return remote(source.at[step, m, at], in_recv.at[step, m, at],
                      red_sem.at[0, step, m, k], red_sem.at[1, step, m, k], inner)

    def send_mid(step, m, k):
        at = chunk_rows(k)
        source = grads if reach == 1 else partial
        return remote(source.at[step, m, at], mid_recv.at[step, m, at],
                      red_sem.at[2, step, m, k], red_sem.at[3, step, m, k], inner)

    def send_out(step, m, k):
        at = whole.at[step, m, chunk_rows(k)]
        return remote(at, at, red_sem.at[4, step, m, k], red_sem.at[5, step, m, k], outer)

    def launch(step, m):
        @pl.when(end)
        def _():
            for k in range(PARTS):
                if reach == 1:
                    send_mid(step, m, k).start()
                else:
                    send_in(step, m, k, grads).start()

    def relay(step, m, k):
        @pl.when(pos > 0)
        def _():
            at = chunk_rows(k)
            send_in(step, m, k, grads).wait_recv()
            total = grads[step, m, at, :].astype(F32) + in_recv[step, m, at, :].astype(F32)
            partial[step, m, at, :] = total.astype(BF16)

            @pl.when(center)
            def _():
                send_mid(step, m, k).start()

            if reach > 2:
                @pl.when(jnp.logical_not(center))
                def _():
                    send_in(step, m, k, partial).start()

    def finish(step, m, k):
        @pl.when(center)
        def _():
            at = chunk_rows(k)
            send_mid(step, m, k).wait_recv()
            source = grads if reach == 1 else partial
            total = source[step, m, at, :].astype(F32) + mid_recv[step, m, at, :].astype(F32)
            whole[step, m, at, :] = total.astype(BF16)
            if reach > 1:
                send_out(step, m, k).start()

    def collect(step, m):
        if reach > 1:
            @pl.when(jnp.logical_not(center))
            def _():
                for k in range(PARTS):
                    send_out(step, m, k).wait_recv()
                    if reach > 2:
                        @pl.when(pos > 0)
                        def _(k=k):
                            send_out(step, m, k).start()

    def drain(step, m):
        for k in range(PARTS):
            @pl.when(center)
            def _(k=k):
                send_mid(step, m, k).wait_send()

            if reach > 1:
                @pl.when(jnp.logical_not(center))
                def _(k=k):
                    send_in(step, m, k, grads).wait_send()

                @pl.when(pos > 0)
                def _(k=k):
                    send_out(step, m, k).wait_send()

    def share_square(step, m):
        return remote(sumsq.at[step, 0, m], sumsq.at[step, 1, m],
                      red_sem.at[6, step, m, 0], red_sem.at[7, step, m, 0], partner)

    def measure(step, m):
        collect(step, m)
        total = jnp.zeros((BLOCK, width), F32)
        for block in range(half // BLOCK):
            part = whole[step, m, block * BLOCK:(block + 1) * BLOCK, :].astype(F32)
            total = total + part * part
        total = total[:8] + total[8:]
        sumsq[step, 0, m] = sum(total[:, j * LANES:(j + 1) * LANES] for j in range(width // LANES))
        share_square(step, m).start()

    def update_memory(step, m):
        share_square(step, m).wait()
        both = sumsq[step, 0, m] + sumsq[step, 1, m]
        frob = jnp.sum(jnp.sum(both, axis=0, keepdims=True), axis=1, keepdims=True)
        scale = STEP_SIZE / jnp.sqrt(frob + EPS)

        def refresh(block):
            at, here = unit_rows(block), block_rows(block)
            update = weights[m, at, :].astype(F32) - scale * whole[step, m, here, :].astype(F32)
            length = jnp.sqrt(jnp.sum(update * update, axis=-1, keepdims=True) + EPS)
            weights[m, at, :] = (update * (target[m, here, :] / length)).astype(BF16)

        each(half // BLOCK, refresh, half // BLOCK)

    def share_memory(m):
        at = weights.at[m, own_units]
        return remote(at, at, w_sem.at[0, m], w_sem.at[1, m], partner)

    def read_copy(g, b):
        there, row = readers(b)
        return remote(ro_send.at[g, b], out_ref.at[g, head * PAIR + col],
                      ro_sem.at[0, g, b], ro_sem.at[1, g, b], device(line, there, core, row))

    def read_block(g, b):
        there, row = readers(b)
        queries = feat[0, g, there * CORES + core, pl.ds(pl.multiple_of(row * quarter, BLOCK), quarter), :]
        hidden, gated = dot_nt(queries, weights[0]), dot_nt(queries, weights[1])
        readmix = (hidden * jax.nn.sigmoid(hidden) * gated).astype(BF16)
        return dot(readmix, weights[2]).astype(BF16)

    def read_ship(g, b):
        ro_send[g, b] = read_block(g, b)
        read_copy(g, b).start()

    def read_keep(g):
        out_ref[g, head * PAIR + col] = read_block(g, last_block)

    def read_ready(g):
        for m in range(3):
            share_memory(m).wait()
        for h in range(HALVES):
            across_copy(g, 0, h).wait()

    strips = 4
    strip = everyone // strips

    def strips_of(i):
        return block_rows(i // strips), pl.ds(pl.multiple_of((i % strips) * strip, LANES), strip)

    def pointwise_first(i):
        at = strips_of(i)
        hidden, gated = hid[at], gat[at]
        sigma = jax.nn.sigmoid(hidden)
        act = hidden * sigma
        mixed[at] = (act * gated).astype(BF16)
        hid[at] = act
        gat[at] = gated * (sigma * (1.0 + hidden * (1.0 - sigma)))

    def pointwise_last(i):
        at = strips_of(i)
        back = bak[at]
        dgate[at] = (back * hid[at]).astype(BF16)
        dfirst[at] = (back * gat[at]).astype(BF16)

    def over_tokens(work):
        each(half // BLOCK * strips, work, strips)

    def group(g):
        settle(g, 1)

        @pl.when(g > 0)
        def _():
            for h in range(HALVES):
                for s in (1, 2):
                    across_copy(g, s, h).wait_send()

        def look():
            pair = weights[0:2, own_units, :].reshape(2 * half, width)
            both = dot_nt(pair, all_tokens(1, g))
            hid[...] = both[:half]
            gat[...] = both[half:]

        def gradient(step, m):
            left, s = ((dfirst, 1), (dgate, 1), (mixed, 2))[m]
            grads[step, m] = dot(left[...], all_tokens(s, g)).astype(BF16)
            launch(step, m)

        orders = ((0, 1, 2), (2, 0, 1))
        chunks = [(step, m, k) for step in range(INNER) for m in orders[step] for k in range(PARTS)]
        per_step = 3 * PARTS

        def relay_at(q):
            relay(*chunks[q])

        def finish_at(q):
            finish(*chunks[q])

        def pass_turn(turn, first, last):
            if turn < last:
                relay_at(turn)
            q = turn - SKEW
            if first <= q < last:
                finish_at(q)
                step, m, k = chunks[q]
                if k == PARTS - 1:
                    measure(step, m)
            if first <= q - LAG < last:
                step, m, k = chunks[q - LAG]
                if k == PARTS - 1:
                    update_memory(step, m)
                    if step == INNER - 1:
                        share_memory(m).start()

        look()
        over_tokens(pointwise_first)
        over_tokens(pointwise_last)
        for m in orders[0]:
            gradient(0, m)

        for turn in range(per_step):
            pass_turn(turn, 0, per_step)
            if turn == 0:
                @pl.when(g > 0)
                def _():
                    read_ready(g - 1)
            if turn <= last_block:
                @pl.when(g > 0)
                def _(turn=turn):
                    if turn < last_block:
                        read_ship(g - 1, turn)
                    else:
                        read_keep(g - 1)
        update_memory(0, 1)
        look()
        finish_at(per_step - 3)
        over_tokens(pointwise_first)
        finish_at(per_step - 2)
        gradient(1, 2)
        finish_at(per_step - 1)
        measure(0, 2)
        for h in range(HALVES):
            across_copy(g, 0, h).start()
        update_memory(0, 2)
        bak[...] = dot_nt(weights[2, own_units, :], all_tokens(2, g))
        relay_at(per_step)
        over_tokens(pointwise_last)
        relay_at(per_step + 1)
        gradient(1, 0)
        relay_at(per_step + 2)
        gradient(1, 1)
        for turn in range(per_step + SKEW, 2 * per_step + SKEW + LAG):
            if turn == 2 * per_step:
                @pl.when(g < groups - 1)
                def _():
                    look_back(g + 1)
            pass_turn(turn, per_step, 2 * per_step)
            if turn == per_step + 7:
                @pl.when(g < groups - 1)
                def _():
                    pass_on(g + 1)
        for step in range(INNER):
            for m in range(3):
                drain(step, m)

    each(groups, group)
    read_ready(groups - 1)
    each(last_block, lambda b: read_ship(groups - 1, b))
    read_keep(groups - 1)

    def land(i):
        read_copy(i // last_block, i % last_block).wait()

    each(groups * last_block, land)


def normalize_kernel(parts_ref, gain_ref, out_ref):
    heads, rows, width = parts_ref.shape[1:]
    for block in range(rows // BLOCK):
        at = slice(block * BLOCK, (block + 1) * BLOCK)
        parts = [parts_ref[0, i, at, :].astype(F32) for i in range(heads)]
        square = jnp.sum(sum(part * part for part in parts), axis=-1, keepdims=True)
        factor = lax.rsqrt(square / (heads * width) + EPS)
        for i, part in enumerate(parts):
            columns = slice(i * width, (i + 1) * width)
            out_ref[0, at, columns] = (part * factor * gain_ref[:, columns]).astype(BF16)


def solution(mesh):
    tok_size, head_size = mesh.shape["tok"], mesh.shape["head"]

    def body(inputs, projections, lrate, fast_init, gain):
        groups, tokens, depth = inputs.shape
        heads, _, units, width = fast_init.shape
        assert heads == PAIR and INNER == 2
        half = units // CORES
        everyone = PAIR * CORES * tokens
        quarter = tokens // head_size
        all_heads = PAIR * head_size
        parts = pl.pallas_call(
            functools.partial(train_kernel, tok_size, head_size),
            out_shape=jax.ShapeDtypeStruct((groups, all_heads, quarter, width), BF16),
            in_specs=[
                pl.BlockSpec(memory_space=pl.ANY),
                pl.BlockSpec(memory_space=pl.ANY),
                pl.BlockSpec(memory_space=pltpu.VMEM),
                pl.BlockSpec(memory_space=pl.ANY),
            ],
            out_specs=pl.BlockSpec(memory_space=pltpu.VMEM),
            scratch_shapes=[
                pltpu.VMEM((groups, tokens, depth), BF16),
                pltpu.VMEM((3, 2, depth, width), BF16),
                pltpu.VMEM((groups, 2, tokens, LANES), F32),
                pltpu.VMEM((3, groups, PAIR * CORES + 1, tokens, width), BF16),
                pltpu.VMEM((3, units, width), BF16),
                pltpu.VMEM((3, half, 1), F32),
                pltpu.VMEM((half, everyone), F32),
                pltpu.VMEM((half, everyone), F32),
                pltpu.VMEM((half, everyone), F32),
                pltpu.VMEM((half, everyone), BF16),
                pltpu.VMEM((half, everyone), BF16),
                pltpu.VMEM((half, everyone), BF16),
                pltpu.VMEM((INNER, 3, half, width), BF16),
                pltpu.VMEM((INNER, 3, half, width), BF16),
                pltpu.VMEM((INNER, 3, half, width), BF16),
                pltpu.VMEM((INNER, 3, half, width), BF16),
                pltpu.VMEM((INNER, 3, half, width), BF16),
                pltpu.VMEM((INNER, 2, 3, 8, LANES), F32),
                pltpu.VMEM((groups, all_heads - 1, quarter, width), BF16),
                pltpu.SemaphoreType.DMA((7 + groups,)),
                pltpu.SemaphoreType.DMA((2, 3, groups, HALVES)),
                pltpu.SemaphoreType.DMA((2, 3, groups, HALVES)),
                pltpu.SemaphoreType.DMA((2, 3, groups, HALVES)),
                pltpu.SemaphoreType.DMA((8, INNER, 3, PARTS)),
                pltpu.SemaphoreType.DMA((2, 3)),
                pltpu.SemaphoreType.DMA((2, groups, all_heads - 1)),
            ],
            compiler_params=pltpu.CompilerParams(
                collective_id=0, has_side_effects=True, vmem_limit_bytes=60000 * 1024
            ),
        )(inputs, projections, lrate.transpose(0, 2, 1), fast_init)
        return pl.pallas_call(
            normalize_kernel,
            grid=(groups, quarter // NORM_ROWS),
            out_shape=jax.ShapeDtypeStruct((groups, quarter, all_heads * width), BF16),
            in_specs=[
                pl.BlockSpec((1, all_heads, NORM_ROWS, width), lambda g, i: (g, 0, i, 0)),
                pl.BlockSpec((1, all_heads * width), lambda g, i: (0, 0)),
            ],
            out_specs=pl.BlockSpec((1, NORM_ROWS, all_heads * width), lambda g, i: (g, i, 0)),
        )(parts, gain[None])

    return jax.shard_map(
        body,
        mesh=mesh,
        in_specs=(
            P(None, "tok", None),
            P(None, None, "head"),
            P(None, "tok", "head"),
            P("head", None, None, None),
            P(),
        ),
        out_specs=P(None, ("tok", "head"), None),
        check_vma=False,
    )
```

```python
import functools

import jax
import jax.numpy as jnp
from jax import lax
from jax.experimental import pallas as pl
from jax.experimental.pallas import tpu as pltpu
from jax.sharding import PartitionSpec as P

INNER = 2
CORES = 2
PAIR = 2
CUTS = (0, 3, 6, 9, 12)
PARTS = len(CUTS) - 1
HALVES = 2
STEP_SIZE = 4.0
EPS = 1e-06
MESH = pl.DeviceIdType.MESH
BLOCK = 16
LANES = 128
NORM_ROWS = 256
SKEW = 3
LAG = 2
NT = (((1,), (1,)), ((), ()))
F32, BF16 = jnp.float32, jnp.bfloat16


def dot(left, right):
    return jnp.dot(left, right, preferred_element_type=F32)


def dot_nt(left, right):
    return lax.dot_general(left, right, NT, preferred_element_type=F32)


def train_kernel(
    tok_size, head_size,
    x_hbm, w_hbm, lr_ref, init_hbm, out_ref,
    x, w, rate, feat, weights, target, hid, gat, bak, mixed, dgate, dfirst,
    grads, in_recv, partial, mid_recv, whole, sumsq, ro_send,
    load_sem, x_sem, own_sem, fwd_sem, red_sem, w_sem, ro_sem,
):
    groups, tokens, depth = x.shape
    units, width = weights.shape[1], weights.shape[2]
    half = units // CORES
    piece = half // CUTS[-1]
    everyone = PAIR * CORES * tokens
    stripe = tokens // HALVES
    quarter = tokens // head_size
    lines = tok_size // (CORES * PAIR)
    reach = lines // 2

    tok, head = lax.axis_index("tok"), lax.axis_index("head")
    core, chip = tok % CORES, tok // CORES
    col, line = chip % PAIR, chip // PAIR
    low = line < reach
    pos = jnp.where(low, line, lines - 1 - line)
    inward = jnp.where(low, 1, -1)
    center, end = pos == reach - 1, pos == 0

    def device(line_, col_, core_, head_):
        return {"tok": (line_ * PAIR + col_) * CORES + core_, "head": head_}

    partner = device(line, col, 1 - core, head)
    across = device(line, 1 - col, core, head)
    inner = device(line + inward, col, core, head)
    outer = device((line - inward + lines) % lines, col, core, head)

    def readers(b):
        dx, dy = 1 - b // head_size, head_size - 1 - b % head_size
        return (col + dx) % PAIR, (head + dy) % head_size

    last_block = PAIR * head_size - 1

    def remote(source, destination, send, recv, to):
        return pltpu.make_async_remote_copy(
            src_ref=source, dst_ref=destination, send_sem=send, recv_sem=recv, device_id=to, device_id_type=MESH
        )

    loads = [pltpu.make_async_copy(x_hbm.at[0], x.at[0], load_sem.at[0])]
    order = [(2, 0), (1, 0), (2, 1), (1, 1), (0, 0), (0, 1)]
    for i, (s, own) in enumerate(order):
        start = pl.multiple_of((col if own else 1 - col) * width, LANES)
        loads.append(pltpu.make_async_copy(
            w_hbm.at[s, :, pl.ds(start, width)], w.at[s, own], load_sem.at[1 + i]))
    for g in range(1, groups):
        loads.append(pltpu.make_async_copy(x_hbm.at[g], x.at[g], load_sem.at[7 + g]))
    own_units = pl.ds(pl.multiple_of(core * half, BLOCK), half)
    load_init = pltpu.make_async_copy(
        init_hbm.at[col, :, own_units], weights.at[:, own_units], load_sem.at[7])
    for copy in loads[:5] + [load_init] + loads[5:]:
        copy.start()

    barrier = pltpu.get_barrier_semaphore()
    pl.semaphore_signal(barrier, inc=1, device_id=partner, device_id_type=MESH)
    pl.semaphore_signal(barrier, inc=1, device_id=inner, device_id_type=MESH)
    for b in range(last_block):
        there, row = readers(b)
        pl.semaphore_signal(barrier, inc=1, device_id=device(line, there, core, row), device_id_type=MESH)
    pl.semaphore_signal(barrier, inc=1, device_id=outer, device_id_type=MESH)

    for g in range(groups):
        for own in range(2):
            which = col if own else 1 - col
            row = lr_ref[g, pl.ds(which, 1), :]
            rate[g, own] = -jnp.transpose(jnp.broadcast_to(row, (LANES, tokens)))

    def stripe_rows(h):
        return pl.ds(pl.multiple_of(h * stripe, stripe), stripe)

    mine, theirs = col * CORES + core, (1 - col) * CORES + core
    parcel = PAIR * CORES

    def project(g, s, own, h):
        rows = stripe_rows(h)
        got = dot(x[g, rows, :], w[s, own]).astype(BF16).astype(F32)
        factor = jnp.where(s == 2, rate[g, own, rows, :], 1.0)
        slot = mine if own else parcel
        for j in range(width // LANES):
            columns = slice(j * LANES, (j + 1) * LANES)
            feat[s, g, slot, rows, columns] = (got[:, columns] * factor).astype(BF16)

    def across_copy(g, s, h):
        rows = stripe_rows(h)
        return remote(feat.at[s, g, parcel, rows], feat.at[s, g, mine, rows],
                      x_sem.at[0, s, g, h], x_sem.at[1, s, g, h], across)

    def own_copy(g, s, h):
        at = feat.at[s, g, mine, stripe_rows(h)]
        return remote(at, at, own_sem.at[0, s, g, h], own_sem.at[1, s, g, h], partner)

    def forward_copy(g, s, h):
        at = feat.at[s, g, theirs, stripe_rows(h)]
        return remote(at, at, fwd_sem.at[0, s, g, h], fwd_sem.at[1, s, g, h], partner)

    def each(count, work, unroll=1):
        def one(i, carry):
            work(i)
            return carry

        lax.fori_loop(0, count, one, 0, unroll=unroll)

    pl.semaphore_wait(barrier, 3 + last_block)
    loads[0].wait()
    for s in (2, 1):
        loads[3 - s].wait()

        def ship_first(h, s=s):
            project(0, s, 0, h)
            across_copy(0, s, h).start()

        each(HALVES, ship_first)

    for copy in loads[3:5]:
        copy.wait()

    def keep_first(i):
        s, h = 2 - i // HALVES, i % HALVES
        project(0, s, 1, h)
        own_copy(0, s, h).start()

    each(2 * HALVES, keep_first)
    load_init.wait()

    def unit_rows(block):
        return pl.ds(pl.multiple_of(core * half + block * BLOCK, BLOCK), BLOCK)

    def block_rows(block):
        return pl.ds(pl.multiple_of(block * BLOCK, BLOCK), BLOCK)

    def prepare(i):
        m, block = i // (half // BLOCK), i % (half // BLOCK)
        start = weights[m, unit_rows(block), :].astype(F32)
        target[m, block_rows(block), :] = jnp.sqrt(jnp.sum(start * start, axis=-1, keepdims=True))

    each(3 * half // BLOCK, prepare, half // BLOCK)
    for copy in loads[5:]:
        copy.wait()

    def ship_rest(i):
        g, j = 1 + i // (2 * HALVES), i % (2 * HALVES)
        project(g, 1 + j % 2, 0, j // 2)

    each((groups - 1) * 2 * HALVES, ship_rest)

    def keep_rest(i):
        g, j = 1 + i // (2 * HALVES), i % (2 * HALVES)
        s, h = 1 + j % 2, j // 2
        project(g, s, 1, h)
        own_copy(g, s, h).start()

    each((groups - 1) * 2 * HALVES, keep_rest)

    def read_other(i):
        project(i // HALVES, 0, 0, i % HALVES)

    def read_own(i):
        project(i // HALVES, 0, 1, i % HALVES)

    each(groups * HALVES, read_other)
    each(groups * HALVES, read_own)

    def pass_on(g):
        for s in (2, 1):
            for h in range(HALVES):
                pass_piece(g, s, h)

    def pass_piece(g, s, h):
        across_copy(g, s, h).wait_recv()
        forward_copy(g, s, h).start()

    def settle(g, s):
        for h in range(HALVES):
            own_copy(g, s, h).wait()
            forward_copy(g, s, h).wait()

    def all_tokens(s, g):
        return feat[s, g, :parcel].reshape(everyone, width)

    def look_back(g):
        settle(g, 2)
        bak[...] = dot_nt(weights[2, own_units, :], all_tokens(2, g))

    for h in range(HALVES):
        pass_piece(0, 2, h)
    for h in range(HALVES - 1):
        pass_piece(0, 1, h)
    look_back(0)
    pass_piece(0, 1, HALVES - 1)
    for h in range(HALVES):
        for s in (1, 2):
            across_copy(0, s, h).wait_send()
    for g in range(1, groups):
        for s in (2, 1):
            for h in range(HALVES):
                across_copy(g, s, h).start()

    def chunk_rows(k):
        return slice(CUTS[k] * piece, CUTS[k + 1] * piece)

    def send_in(step, m, k, source):
        at = chunk_rows(k)
        return remote(source.at[step, m, at], in_recv.at[step, m, at],
                      red_sem.at[0, step, m, k], red_sem.at[1, step, m, k], inner)

    def send_mid(step, m, k):
        at = chunk_rows(k)
        source = grads if reach == 1 else partial
        return remote(source.at[step, m, at], mid_recv.at[step, m, at],
                      red_sem.at[2, step, m, k], red_sem.at[3, step, m, k], inner)

    def send_out(step, m, k):
        at = whole.at[step, m, chunk_rows(k)]
        return remote(at, at, red_sem.at[4, step, m, k], red_sem.at[5, step, m, k], outer)

    def launch(step, m):
        @pl.when(end)
        def _():
            for k in range(PARTS):
                if reach == 1:
                    send_mid(step, m, k).start()
                else:
                    send_in(step, m, k, grads).start()

    def relay(step, m, k):
        @pl.when(pos > 0)
        def _():
            at = chunk_rows(k)
            send_in(step, m, k, grads).wait_recv()
            total = grads[step, m, at, :].astype(F32) + in_recv[step, m, at, :].astype(F32)
            partial[step, m, at, :] = total.astype(BF16)

            @pl.when(center)
            def _():
                send_mid(step, m, k).start()

            if reach > 2:
                @pl.when(jnp.logical_not(center))
                def _():
                    send_in(step, m, k, partial).start()

    def finish(step, m, k):
        @pl.when(center)
        def _():
            at = chunk_rows(k)
            send_mid(step, m, k).wait_recv()
            source = grads if reach == 1 else partial
            total = source[step, m, at, :].astype(F32) + mid_recv[step, m, at, :].astype(F32)
            whole[step, m, at, :] = total.astype(BF16)
            if reach > 1:
                send_out(step, m, k).start()

    def collect(step, m):
        if reach > 1:
            @pl.when(jnp.logical_not(center))
            def _():
                for k in range(PARTS):
                    send_out(step, m, k).wait_recv()
                    if reach > 2:
                        @pl.when(pos > 0)
                        def _(k=k):
                            send_out(step, m, k).start()

    def drain(step, m):
        for k in range(PARTS):
            @pl.when(center)
            def _(k=k):
                send_mid(step, m, k).wait_send()

            if reach > 1:
                @pl.when(jnp.logical_not(center))
                def _(k=k):
                    send_in(step, m, k, grads).wait_send()

                @pl.when(pos > 0)
                def _(k=k):
                    send_out(step, m, k).wait_send()

    def share_square(step, m):
        return remote(sumsq.at[step, 0, m], sumsq.at[step, 1, m],
                      red_sem.at[6, step, m, 0], red_sem.at[7, step, m, 0], partner)

    def measure(step, m):
        collect(step, m)
        total = jnp.zeros((BLOCK, width), F32)
        for block in range(half // BLOCK):
            part = whole[step, m, block * BLOCK:(block + 1) * BLOCK, :].astype(F32)
            total = total + part * part
        total = total[:8] + total[8:]
        sumsq[step, 0, m] = sum(total[:, j * LANES:(j + 1) * LANES] for j in range(width // LANES))
        share_square(step, m).start()

    def update_memory(step, m):
        share_square(step, m).wait()
        both = sumsq[step, 0, m] + sumsq[step, 1, m]
        frob = jnp.sum(jnp.sum(both, axis=0, keepdims=True), axis=1, keepdims=True)
        scale = STEP_SIZE / jnp.sqrt(frob + EPS)

        def refresh(block):
            at, here = unit_rows(block), block_rows(block)
            update = weights[m, at, :].astype(F32) - scale * whole[step, m, here, :].astype(F32)
            length = jnp.sqrt(jnp.sum(update * update, axis=-1, keepdims=True) + EPS)
            weights[m, at, :] = (update * (target[m, here, :] / length)).astype(BF16)

        each(half // BLOCK, refresh, half // BLOCK)

    def share_memory(m):
        at = weights.at[m, own_units]
        return remote(at, at, w_sem.at[0, m], w_sem.at[1, m], partner)

    def read_copy(g, b):
        there, row = readers(b)
        return remote(ro_send.at[g, b], out_ref.at[g, head * PAIR + col],
                      ro_sem.at[0, g, b], ro_sem.at[1, g, b], device(line, there, core, row))

    def read_block(g, b):
        there, row = readers(b)
        queries = feat[0, g, there * CORES + core, pl.ds(pl.multiple_of(row * quarter, BLOCK), quarter), :]
        hidden, gated = dot_nt(queries, weights[0]), dot_nt(queries, weights[1])
        readmix = (hidden * jax.nn.sigmoid(hidden) * gated).astype(BF16)
        return dot(readmix, weights[2]).astype(BF16)

    def read_ship(g, b):
        ro_send[g, b] = read_block(g, b)
        read_copy(g, b).start()

    def read_keep(g):
        out_ref[g, head * PAIR + col] = read_block(g, last_block)

    def read_ready(g):
        for m in range(3):
            share_memory(m).wait()
        for h in range(HALVES):
            across_copy(g, 0, h).wait()

    strips = 4
    strip = everyone // strips

    def strips_of(i):
        return block_rows(i // strips), pl.ds(pl.multiple_of((i % strips) * strip, LANES), strip)

    def pointwise_first(i):
        at = strips_of(i)
        hidden, gated = hid[at], gat[at]
        sigma = jax.nn.sigmoid(hidden)
        act = hidden * sigma
        mixed[at] = (act * gated).astype(BF16)
        hid[at] = act
        gat[at] = gated * (sigma * (1.0 + hidden * (1.0 - sigma)))

    def pointwise_last(i):
        at = strips_of(i)
        back = bak[at]
        dgate[at] = (back * hid[at]).astype(BF16)
        dfirst[at] = (back * gat[at]).astype(BF16)

    def over_tokens(work):
        each(half // BLOCK * strips, work, strips)

    def group(g):
        settle(g, 1)

        @pl.when(g > 0)
        def _():
            for h in range(HALVES):
                for s in (1, 2):
                    across_copy(g, s, h).wait_send()

        def look():
            pair = weights[0:2, own_units, :].reshape(2 * half, width)
            both = dot_nt(pair, all_tokens(1, g))
            hid[...] = both[:half]
            gat[...] = both[half:]

        def gradient(step, m):
            left, s = ((dfirst, 1), (dgate, 1), (mixed, 2))[m]
            grads[step, m] = dot(left[...], all_tokens(s, g)).astype(BF16)
            launch(step, m)

        orders = ((0, 1, 2), (2, 0, 1))
        chunks = [(step, m, k) for step in range(INNER) for m in orders[step] for k in range(PARTS)]
        per_step = 3 * PARTS

        def relay_at(q):
            relay(*chunks[q])

        def finish_at(q):
            finish(*chunks[q])

        def pass_turn(turn, first, last):
            if turn < last:
                relay_at(turn)
            q = turn - SKEW
            if first <= q < last:
                finish_at(q)
                step, m, k = chunks[q]
                if k == PARTS - 1:
                    measure(step, m)
            if first <= q - LAG < last:
                step, m, k = chunks[q - LAG]
                if k == PARTS - 1:
                    update_memory(step, m)
                    if step == INNER - 1:
                        share_memory(m).start()

        look()
        over_tokens(pointwise_first)
        over_tokens(pointwise_last)
        for m in orders[0]:
            gradient(0, m)

        for turn in range(per_step):
            pass_turn(turn, 0, per_step)
            if turn == 0:
                @pl.when(g > 0)
                def _():
                    read_ready(g - 1)
            if turn % 2 == 0 and turn // 2 <= last_block:
                @pl.when(g > 0)
                def _(b=turn // 2):
                    if b < last_block:
                        read_ship(g - 1, b)
                    else:
                        read_keep(g - 1)
        update_memory(0, 1)
        look()
        finish_at(per_step - 3)
        over_tokens(pointwise_first)
        finish_at(per_step - 2)
        gradient(1, 2)
        finish_at(per_step - 1)
        measure(0, 2)
        for h in range(HALVES):
            across_copy(g, 0, h).start()
        update_memory(0, 2)
        bak[...] = dot_nt(weights[2, own_units, :], all_tokens(2, g))
        relay_at(per_step)
        over_tokens(pointwise_last)
        relay_at(per_step + 1)
        gradient(1, 0)
        relay_at(per_step + 2)
        gradient(1, 1)
        for turn in range(per_step + SKEW, 2 * per_step + SKEW + LAG):
            if turn == 2 * per_step:
                @pl.when(g < groups - 1)
                def _():
                    look_back(g + 1)
            pass_turn(turn, per_step, 2 * per_step)
            if turn == per_step + 7:
                @pl.when(g < groups - 1)
                def _():
                    pass_on(g + 1)
        for step in range(INNER):
            for m in range(3):
                drain(step, m)

    each(groups, group)
    read_ready(groups - 1)
    each(last_block, lambda b: read_ship(groups - 1, b))
    read_keep(groups - 1)

    def land(i):
        read_copy(i // last_block, i % last_block).wait()

    each(groups * last_block, land)


def normalize_kernel(parts_ref, gain_ref, out_ref):
    heads, rows, width = parts_ref.shape[1:]
    for block in range(rows // BLOCK):
        at = slice(block * BLOCK, (block + 1) * BLOCK)
        parts = [parts_ref[0, i, at, :].astype(F32) for i in range(heads)]
        square = jnp.sum(sum(part * part for part in parts), axis=-1, keepdims=True)
        factor = lax.rsqrt(square / (heads * width) + EPS)
        for i, part in enumerate(parts):
            columns = slice(i * width, (i + 1) * width)
            out_ref[0, at, columns] = (part * factor * gain_ref[:, columns]).astype(BF16)


def solution(mesh):
    tok_size, head_size = mesh.shape["tok"], mesh.shape["head"]

    def body(inputs, projections, lrate, fast_init, gain):
        groups, tokens, depth = inputs.shape
        heads, _, units, width = fast_init.shape
        assert heads == PAIR and INNER == 2
        half = units // CORES
        everyone = PAIR * CORES * tokens
        quarter = tokens // head_size
        all_heads = PAIR * head_size
        parts = pl.pallas_call(
            functools.partial(train_kernel, tok_size, head_size),
            out_shape=jax.ShapeDtypeStruct((groups, all_heads, quarter, width), BF16),
            in_specs=[
                pl.BlockSpec(memory_space=pl.ANY),
                pl.BlockSpec(memory_space=pl.ANY),
                pl.BlockSpec(memory_space=pltpu.VMEM),
                pl.BlockSpec(memory_space=pl.ANY),
            ],
            out_specs=pl.BlockSpec(memory_space=pltpu.VMEM),
            scratch_shapes=[
                pltpu.VMEM((groups, tokens, depth), BF16),
                pltpu.VMEM((3, 2, depth, width), BF16),
                pltpu.VMEM((groups, 2, tokens, LANES), F32),
                pltpu.VMEM((3, groups, PAIR * CORES + 1, tokens, width), BF16),
                pltpu.VMEM((3, units, width), BF16),
                pltpu.VMEM((3, half, 1), F32),
                pltpu.VMEM((half, everyone), F32),
                pltpu.VMEM((half, everyone), F32),
                pltpu.VMEM((half, everyone), F32),
                pltpu.VMEM((half, everyone), BF16),
                pltpu.VMEM((half, everyone), BF16),
                pltpu.VMEM((half, everyone), BF16),
                pltpu.VMEM((INNER, 3, half, width), BF16),
                pltpu.VMEM((INNER, 3, half, width), BF16),
                pltpu.VMEM((INNER, 3, half, width), BF16),
                pltpu.VMEM((INNER, 3, half, width), BF16),
                pltpu.VMEM((INNER, 3, half, width), BF16),
                pltpu.VMEM((INNER, 2, 3, 8, LANES), F32),
                pltpu.VMEM((groups, all_heads - 1, quarter, width), BF16),
                pltpu.SemaphoreType.DMA((7 + groups,)),
                pltpu.SemaphoreType.DMA((2, 3, groups, HALVES)),
                pltpu.SemaphoreType.DMA((2, 3, groups, HALVES)),
                pltpu.SemaphoreType.DMA((2, 3, groups, HALVES)),
                pltpu.SemaphoreType.DMA((8, INNER, 3, PARTS)),
                pltpu.SemaphoreType.DMA((2, 3)),
                pltpu.SemaphoreType.DMA((2, groups, all_heads - 1)),
            ],
            compiler_params=pltpu.CompilerParams(
                collective_id=0, has_side_effects=True, vmem_limit_bytes=60000 * 1024
            ),
        )(inputs, projections, lrate.transpose(0, 2, 1), fast_init)
        return pl.pallas_call(
            normalize_kernel,
            grid=(groups, quarter // NORM_ROWS),
            out_shape=jax.ShapeDtypeStruct((groups, quarter, all_heads * width), BF16),
            in_specs=[
                pl.BlockSpec((1, all_heads, NORM_ROWS, width), lambda g, i: (g, 0, i, 0)),
                pl.BlockSpec((1, all_heads * width), lambda g, i: (0, 0)),
            ],
            out_specs=pl.BlockSpec((1, NORM_ROWS, all_heads * width), lambda g, i: (g, i, 0)),
        )(parts, gain[None])

    return jax.shard_map(
        body,
        mesh=mesh,
        in_specs=(
            P(None, "tok", None),
            P(None, None, "head"),
            P(None, "tok", "head"),
            P("head", None, None, None),
            P(),
        ),
        out_specs=P(None, ("tok", "head"), None),
        check_vma=False,
    )
```
